32 devices in a mesh: rep: 2 (over x), dp: 16 (over y, z, core).
Axes of the slice: x: 2, y: 2, z: 4, core: 2. Of those that a mesh axis runs over, the one named last changes fastest.
Arguments:
- x: bfloat16 [32, 1024, 1024], P(('rep', 'dp')), parts along dimension 0
- dy: bfloat16 [32, 1024, 1024], P(('rep', 'dp')), parts along dimension 0
- wq: bfloat16 [2, 1024, 1024], P(None, 'dp')
- wk: bfloat16 [2, 1024, 256], P(None, 'dp')
- wv: bfloat16 [2, 1024, 256], P(None, 'dp')
- wo: bfloat16 [2, 1024, 1024], P(None, 'dp')
- w_gate: bfloat16 [2, 1024, 3200], P(None, 'dp')
- w_up: bfloat16 [2, 1024, 3200], P(None, 'dp')
- w_down: bfloat16 [2, 3200, 1024], P(None, 'dp')
Outputs:
- output 1: bfloat16 [32, 1024, 1024], P(('rep', 'dp')), parts along dimension 0
- output 2: bfloat16 [4, 1024, 1024], P('rep', 'dp'), parts along dimension 0
- output 3: bfloat16 [4, 1024, 256], P('rep', 'dp'), parts along dimension 0
- output 4: bfloat16 [4, 1024, 256], P('rep', 'dp'), parts along dimension 0
- output 5: bfloat16 [4, 1024, 1024], P('rep', 'dp'), parts along dimension 0
- output 6: bfloat16 [4, 1024, 3200], P('rep', 'dp'), parts along dimension 0
- output 7: bfloat16 [4, 1024, 3200], P('rep', 'dp'), parts along dimension 0
- output 8: bfloat16 [4, 3200, 1024], P('rep', 'dp'), parts along dimension 0
There are 2 independent parts. The reference program is written for one: setup_inputs(seed, part) draws one part's arguments, and reference() takes and returns one part's arrays. A program takes and returns all parts, laid end to end along the dimension named above; an argument that names none is the same for every part.
All inputs are finite; a program needn't handle non-finite values.
Results may differ from the reference program's by a relative error of at most 0.0301.
Values are sent between devices in bfloat16 or wider.
A program may use at most 2 GiB of HBM per device.

```python
import jax
import jax.numpy as jnp
from jax import lax

SEQUENCES = 16
TOKENS = 1024
D = 1024
HEADS = 8
KV_HEADS = 2
HEAD = 128
FF = 3200
LAYERS = 2
THETA = 10000
NAMES = ("wq", "wk", "wv", "wo", "w_gate", "w_up", "w_down")
SHAPES = {
    "wq": (LAYERS, D, HEADS * HEAD),
    "wk": (LAYERS, D, KV_HEADS * HEAD),
    "wv": (LAYERS, D, KV_HEADS * HEAD),
    "wo": (LAYERS, HEADS * HEAD, D),
    "w_gate": (LAYERS, D, FF),
    "w_up": (LAYERS, D, FF),
    "w_down": (LAYERS, FF, D),
}


def bump(key, n, height):
    away = (jnp.arange(n, dtype=jnp.int32) - jax.random.randint(key, (), 0, n, jnp.int32)) % n
    return jnp.where(away < n // 8, height, 1.0)


def together(key, own, strength):
    shared = jax.random.normal(key, own.shape[1:], jnp.float32)
    return (own + strength * shared) * lax.rsqrt(1 + strength * strength)


def setup_inputs(seed: int = 0, part: int = 0) -> dict:
    kx, kdy, ka, kb, kz, kf, kh, kl, *keys = jax.random.split(jax.random.key(seed), 8 + 3 * len(NAMES))
    kx, kdy, ka, kb = (jax.random.fold_in(k, part) for k in (kx, kdy, ka, kb))
    kw, km, kv = (keys[i::3] for i in range(3))
    shape = (SEQUENCES, TOKENS, D)
    much_x, much_dy = jax.random.uniform(kz, (2,), jnp.float32, 0.0, 1.0)
    loud = 2.0 ** jax.random.uniform(jax.random.fold_in(kz, 1), (), jnp.float32, -1.0, 2.0)
    layers = 2.0 ** jax.random.uniform(kl, (LAYERS, 1, 1), jnp.float32, -1.0, 1.0)
    times = {"wq": 1.0, "wk": 1.0, "wv": 2.0, "wo": layers, "w_gate": 1.0, "w_up": bump(kh, FF, 4.0), "w_down": layers}
    x = together(ka, jax.random.normal(kx, shape, jnp.float32), much_x) * bump(kf, D, 4.0)
    dy = together(kb, jax.random.normal(kdy, shape, jnp.float32), much_dy)
    drawn = {"x": x.astype(jnp.bfloat16), "dy": (loud * dy * (SEQUENCES * TOKENS) ** -0.5).astype(jnp.bfloat16)}
    for key, name in zip(kw, NAMES, strict=True):
        drawn[name] = (jax.random.normal(key, SHAPES[name], jnp.float32) * SHAPES[name][1] ** -0.5 * times[name]).astype(jnp.bfloat16)
    return drawn


def matmul(a, w):
    return jnp.dot(a, w, preferred_element_type=jnp.float32).astype(jnp.bfloat16)


def normed(h):
    wide = h.astype(jnp.float32)
    scale = lax.rsqrt(jnp.mean(wide**2, -1, keepdims=True) + 1e-6)
    return (wide * scale).astype(jnp.bfloat16)


def turned(t, theta):
    half = t.shape[-1] // 2
    angle = jnp.arange(t.shape[0], dtype=jnp.float32)[:, None] * theta ** (-jnp.arange(half, dtype=jnp.float32) / half)
    cos, sin = jnp.cos(angle)[:, None], jnp.sin(angle)[:, None]
    a, b = t[..., :half].astype(jnp.float32), t[..., half:].astype(jnp.float32)
    return jnp.concatenate([a * cos - b * sin, b * cos + a * sin], -1).astype(jnp.bfloat16)


def seen_by(q, k, v):
    tokens, kv = q.shape[0], k.shape[1]
    q = q.reshape(tokens, kv, -1, q.shape[-1])
    scores = jnp.einsum("tgsd,ugd->gstu", q.astype(jnp.float32), k.astype(jnp.float32)) * q.shape[-1] ** -0.5
    place = jnp.arange(tokens)
    weights = jax.nn.softmax(jnp.where(place[:, None] >= place, scores, -jnp.inf), -1).astype(jnp.bfloat16)
    return jnp.einsum("gstu,ugd->tgsd", weights.astype(jnp.float32), v.astype(jnp.float32)).astype(jnp.bfloat16).reshape(tokens, -1)


def layer(h, w):
    a = normed(h)
    q, k = (turned(matmul(a, w[name]).reshape(h.shape[0], -1, HEAD), THETA) for name in ("wq", "wk"))
    h = h + matmul(seen_by(q, k, matmul(a, w["wv"]).reshape(h.shape[0], -1, HEAD)), w["wo"])
    b = normed(h)
    gate = jnp.dot(b, w["w_gate"], preferred_element_type=jnp.float32)
    up = jnp.dot(b, w["w_up"], preferred_element_type=jnp.float32)
    return h + matmul((jax.nn.silu(gate) * up).astype(jnp.bfloat16), w["w_down"])


def stack(weights, h):
    return lax.scan(lambda h, w: (layer(h, w), None), h, weights)[0]


def reference(x, dy, wq, wk, wv, wo, w_gate, w_up, w_down):
    weights = dict(zip(NAMES, (wq, wk, wv, wo, w_gate, w_up, w_down), strict=True))

    def take(so_far, sequence):
        h, by_y = sequence
        _, back = jax.vjp(stack, weights, h)
        by_weights, by_h = back(by_y)
        return jax.tree.map(lambda total, term: total + term.astype(jnp.float32), so_far, by_weights), by_h

    none_yet = {name: jnp.zeros(w.shape, jnp.float32) for name, w in weights.items()}
    by_weights, by_x = lax.scan(take, none_yet, (x, dy))
    return (by_x, *(by_weights[name].astype(jnp.bfloat16) for name in NAMES))
```

```python
import functools

import jax
import jax.numpy as jnp
from jax import lax
from jax.experimental import pallas as pl
from jax.experimental.pallas import tpu as pltpu
from jax.sharding import PartitionSpec as P

bf16, f32 = jnp.bfloat16, jnp.float32
SEM = pltpu.SemaphoreType.DMA


def nn(a, b):
    return lax.dot_general(a, b, (((1,), (0,)), ((), ())), preferred_element_type=f32)


def nt(a, b):
    return lax.dot_general(a, b, (((1,), (1,)), ((), ())), preferred_element_type=f32)


def tn(a, b):
    return lax.dot_general(a, b, (((0,), (0,)), ((), ())), preferred_element_type=f32)


def where_am_i():
    return tuple(lax.axis_index(name) for name in ("x", "y", "z", "c"))


def peer(**there):
    at = dict(zip(("x", "y", "z", "c"), where_am_i()), **there)
    return at["x"], at["y"], at["z"], at["c"]


def greet(peers):
    barrier = pltpu.get_barrier_semaphore()
    for there in peers:
        pl.semaphore_signal(barrier, inc=1, device_id=peer(**there), device_id_type=pl.DeviceIdType.MESH)
    pl.semaphore_wait(barrier, len(peers))


def norm_back(g, wide):
    scale = lax.rsqrt(jnp.mean(wide * wide, -1, keepdims=True) + 1e-6)
    return g * scale - wide * (scale * scale * scale * jnp.mean(g * wide, -1, keepdims=True))


HEADS, GROUPS, HEAD = 4, 2, 128
PART = (HEADS + 2) * HEAD
BQ = 256
SCALE = HEAD**-0.5
LOG2E = 1.4426950408889634


PER_STEP = 2
LAGS = (0, 1, 2, 3)
V_AT = (HEADS + 1) * HEAD


def params(number):
    return pltpu.CompilerParams(collective_id=number, has_side_effects=True, vmem_limit_bytes=63 * 2**20)


def tiles(rows, size=512):
    def run(body):
        @pl.loop(0, rows // size)
        def _(t):
            body(pl.ds(pl.multiple_of(t * size, size), size))
    return run


def norm(wide):
    return (wide * lax.rsqrt(jnp.mean(wide * wide, -1, keepdims=True) + 1e-6)).astype(bf16)


def attend_block(qkv, att, lse, iq):
    for g in range(GROUPS):
        rows, seen, first = slice(iq * BQ, (iq + 1) * BQ), (iq + 1) * BQ, g * PART
        k, v = qkv[:seen, first + V_AT - HEAD : first + V_AT], qkv[:seen, first + V_AT : first + PART]
        for n in range(0, HEADS, 2):
            q = jnp.concatenate([qkv[rows, first + i * HEAD : first + (i + 1) * HEAD] for i in (n, n + 1)], axis=0)
            s = nt(k, q)
            gap = lax.rem(lax.broadcasted_iota(jnp.int32, (BQ, 2 * BQ), 1), BQ) - lax.broadcasted_iota(jnp.int32, (BQ, 2 * BQ), 0)
            last = jnp.where(gap >= 0, s[iq * BQ :], -1e30)
            s = jnp.concatenate([s[: iq * BQ], last], axis=0) if iq else last
            top = s.max(0, keepdims=True)
            p = jnp.exp2((s - top) * (SCALE * LOG2E))
            total = p.sum(0, keepdims=True)
            out = tn(v, p.astype(bf16)) * (1 / total)
            stat = top * SCALE + jnp.log(total)
            for i in (0, 1):
                head = g * HEADS + n + i
                att[rows, head * HEAD : (head + 1) * HEAD] = out[:, i * BQ : (i + 1) * BQ].T.astype(bf16)
                lse[head : head + 1, rows] = stat[:, i * BQ : (i + 1) * BQ]


def chip_bits(y, z):
    return [y, lax.div(z, 2), lax.rem(z, 2)]


def partner(bits, bit):
    y, high, low = bits
    return [{"y": 1 - y}, {"z": (1 - high) * 2 + low}, {"z": high * 2 + 1 - low}][bit]


class Sums:
    ORDERS = ((0, 2, 1), (2, 0, 1))
    REFS = 13
    SHARE = 4

    @classmethod
    def places_for(cls, lag):
        return 2 * lag + cls.SHARE - 1

    @classmethod
    def scratch(cls, rows, width, lag, stored=None):
        halves = [(n, size, rows, width) for n, size in zip(lag, (4, 2, 1))]
        return [
            pltpu.VMEM((2, 16 * rows, stored or width), f32),
            *(pltpu.VMEM((2, 8, rows, width), bf16) for _ in range(2)),
            *(pltpu.VMEM(s, f32) for s in halves),
            *(pltpu.VMEM(s, bf16) for s in halves),
            *(pltpu.VMEM((cls.places_for(s[0]), *s[1:]), bf16) for s in halves),
            SEM((4, 2, cls.places_for(max(lag)))),
        ]

    def __init__(self, refs, rows, width, lag):
        self.term, self.c_out, self.c_in, *rest, self.sem = refs
        self.keep, self.out, self.into = rest[:3], rest[3:6], rest[6:]
        self.rows, self.width, self.lag = rows, width, lag
        _, y, z, self.c = where_am_i()
        self.bits = chip_bits(y, z)

    def slot(self, i, stage):
        return i % (2 if stage == 0 else self.lag[stage - 1])

    def landing(self, i, stage):
        return i % (2 if stage == 0 else self.places_for(self.lag[stage - 1]))

    def order(self, i):
        return self.ORDERS[1 if i % self.SHARE == self.SHARE - 1 else 0]

    def partner(self, bit):
        return partner(self.bits, bit)

    def greet(self):
        greet([{"c": 1 - self.c}] + [partner(self.bits, bit) for bit in self.ORDERS[0]])

    def copy(self, i, stage):
        s = self.slot(i, stage)
        d = self.landing(i, stage)
        src, dst = (self.c_out, self.c_in) if stage == 0 else (self.out[stage - 1], self.into[stage - 1])
        to = {"c": 1 - self.c} if stage == 0 else self.partner(self.order(i)[stage - 1])
        return pltpu.make_async_remote_copy(src.at[s], dst.at[d], self.sem.at[stage, 0, s], self.sem.at[stage, 1, d],
                                            device_id=peer(**to), device_id_type=pl.DeviceIdType.MESH)

    def block(self, k, c, at):
        slot, column = at
        return self.term[slot, pl.ds(pl.multiple_of((2 * k + c) * self.rows, 8), self.rows), column : column + self.width]

    def to_core(self, i, at):
        if i >= 2:
            self.copy(i - 2, 0).wait_send()

        @pl.loop(0, 8)
        def _(k):
            self.c_out[i % 2, k] = self.block(k, 1 - self.c, at).astype(bf16)

        self.copy(i, 0).start()

    def places(self, i, stage, side):
        order = self.order(i)
        left = sorted(order[stage - 1 :])
        bit = order[stage - 1]
        mine = self.bits[bit]
        want = mine if side == 0 else 1 - mine
        rest = [b for b in left if b != bit]
        out = []
        for n in range(2 ** len(rest)):
            value = {b: (n >> (len(rest) - 1 - j)) & 1 for j, b in enumerate(rest)}
            value[bit] = want
            k = 0
            for b in left:
                k = k * 2 + value[b]
            out.append(k)
        return out

    def to_chip(self, i, stage, at=None):
        s, before, came = self.slot(i, stage), self.slot(i, stage - 1), self.landing(i, stage - 1)
        if i >= self.lag[stage - 1]:
            self.copy(i - self.lag[stage - 1], stage).wait_send()
        self.copy(i, stage - 1).wait_recv()

        def value(k):
            if stage == 1:
                return self.block(k, self.c, at) + self.c_in[came, k].astype(f32)
            return self.keep[stage - 2][before, k] + self.into[stage - 2][came, k].astype(f32)

        for n, k in enumerate(self.places(i, stage, 1)):
            self.out[stage - 1][s, n] = value(k).astype(bf16)
        for n, k in enumerate(self.places(i, stage, 0)):
            self.keep[stage - 1][s, n] = value(k)
        self.copy(i, stage).start()

    def total(self, i):
        self.copy(i, 3).wait_recv()
        return self.keep[2][self.slot(i, 3), 0] + self.into[2][self.landing(i, 3), 0].astype(f32)

    def finish(self, count):
        for stage in range(4):
            for i in range(max(count - (2 if stage == 0 else self.lag[stage - 1]), 0), count):
                self.copy(i, stage).wait_send()


def pipeline(items, lag):
    n = len(items)
    a, b, c = lag
    starts = {1: 1, 2: 1 + a, 3: 1 + a + b, 4: 1 + a + b + c}
    for t in range(n + starts[4]):
        for stage in (4, 3, 2):
            if 0 <= t - starts[stage] < n and len(items[t - starts[stage]]) > 1:
                _, sums, i, _, store = items[t - starts[stage]]
                if stage == 4:
                    store(sums.total(i).astype(bf16))
                else:
                    sums.to_chip(i, stage)
        if t < n:
            items[t][0]()
        if 0 <= t - 1 < n and len(items[t - 1]) > 1:
            _, sums, i, at, _ = items[t - 1]
            sums.to_chip(i, 1, at)
        if t < n and len(items[t]) > 1:
            _, sums, i, at, _ = items[t]
            sums.to_core(i, at)


BLOCKS, CHUNK, DW, WIDE = 16, 512, 128, 256
FFN_LAG, ATT_LAG = (6, 5, 4), (3, 3, 2)


def ffn_back_kernel(dh_h, b_h, mid_h, m_h, wg_h, wu_h, wd_h, dmid_h, gd_h, gg_h, gu_h, dh, b, bt, m, mt, wg, wu, wd, db, dgate, dup, ends, gd, gg, gu,
                    in_sem, m_sem, w_sem, out_sem, *sums):
    T, D = b.shape
    F = mt.shape[0]
    chunks = [(at, min(CHUNK, F - at)) for at in range(0, F, CHUNK)]
    down = Sums(sums[: Sums.REFS], F // BLOCKS, DW, FFN_LAG)
    wide = Sums(sums[Sums.REFS :], D // BLOCKS, WIDE, FFN_LAG)
    MT = m.shape[2]

    def w_copies(j):
        s, (at, w) = j % 2, chunks[j]
        pairs = ((wg_h.at[:, pl.ds(at, w)], wg.at[s, :, pl.ds(0, w)]), (wu_h.at[:, pl.ds(at, w)], wu.at[s, :, pl.ds(0, w)]),
                 (wd_h.at[pl.ds(at, w), :], wd.at[s, pl.ds(0, w), :]))
        return [pltpu.make_async_copy(src, dst, w_sem.at[n, s]) for n, (src, dst) in enumerate(pairs)]

    def m_copy(j):
        return pltpu.make_async_copy(m_h.at[:, pl.ds(j * MT, MT)], m.at[j % 2], m_sem.at[j % 2])

    loads = [pltpu.make_async_copy(src, dst, in_sem.at[n]) for n, (src, dst) in enumerate(((dh_h, dh), (b_h, b)))]
    m_copy(0).start()
    for load in loads:
        load.start()
    m_copy(1).start()
    for copy in w_copies(0):
        copy.start()
    down.greet()

    def down_term(i):
        def run():
            if i % 2:
                return
            cols = slice(i * DW, (i + 2) * DW)
            if i == 0:
                loads[0].wait()
                for j in range(F // MT):
                    m_copy(j).wait()
                    mt[j * MT : (j + 1) * MT, :] = m[j % 2].T
                    if j + 2 < F // MT:
                        m_copy(j + 2).start()
                    down.term[0, j * MT : (j + 1) * MT, :] = nn(mt[j * MT : (j + 1) * MT, :], dh[:, cols])
                return

            @tiles(F, MT)
            def _(rows):
                down.term[i // 2 % 2, rows, :] = nn(mt[rows, :], dh[:, cols])
        return run

    def down_store(i):
        def run(total):
            gd[:, i * DW : (i + 1) * DW] = total
        return run

    def chunk(j):
        s, (at, w) = j % 2, chunks[j]
        if j == 0:
            loads[1].wait()
            bt[...] = b[...].T
        if j + 1 < len(chunks):
            for copy in w_copies(j + 1):
                copy.start()
        for copy in w_copies(j):
            copy.wait()

        @tiles(T)
        def _(rows):
            dm = nt(dh[rows, :], wd[s, :w, :]).astype(bf16).astype(f32)
            gate, up = nn(b[rows, :], wg[s, :, :w]), nn(b[rows, :], wu[s, :, :w])
            sig = 1 / (1 + jnp.exp(-gate))
            to_up = (dm * (gate * sig)).astype(bf16)
            to_gate = (dm * up * (sig * (1 + gate * (1 - sig)))).astype(bf16)
            if w == CHUNK:
                dup[rows, :] = to_up
                dgate[rows, :] = to_gate
            else:
                ends[rows, :w] = to_gate
                ends[rows, w:] = to_up
            term = nt(to_gate, wg[s, :, :w]) + nt(to_up, wu[s, :, :w])
            if j == 0:
                db[rows, :] = term
            else:
                db[rows, :] += term

    def wide_term(j, which, piece, n):
        def run():
            if which == 0 and piece == 0:
                chunk(j)
            right = ends[...] if chunks[j][1] < CHUNK else (dgate, dup)[which][:, piece * WIDE : (piece + 1) * WIDE]

            @tiles(D)
            def _(rows):
                wide.term[n % 2, rows, :] = nn(bt[rows, :], right)
        return run

    def wide_store(j, which, piece):
        at, w = chunks[j]

        def run(total):
            if w < CHUNK:
                gg[:, at : at + w] = total[:, :w]
                gu[:, at : at + w] = total[:, w:]
            else:
                (gg, gu)[which][:, at + piece * WIDE : at + (piece + 1) * WIDE] = total
        return run

    items = [(down_term(i), down, i, (i // 2 % 2, i % 2 * DW), down_store(i)) for i in range(D // DW)]
    n = 0
    for j, (at, w) in enumerate(chunks):
        for which, piece in [(which, piece) for which in (0, 1) for piece in range(CHUNK // WIDE)] if w == CHUNK else [(0, 0)]:
            items.append((wide_term(j, which, piece, n), wide, n, (n % 2, 0), wide_store(j, which, piece)))
            n += 1
    mid = b
    pipeline(items, FFN_LAG)
    load_mid = pltpu.make_async_copy(mid_h, mid, in_sem.at[0])
    load_mid.start()
    load_mid.wait()

    @tiles(T)
    def _(rows):
        g = norm_back(db[rows, :].astype(bf16).astype(f32), mid[rows, :].astype(f32))
        dh[rows, :] = (dh[rows, :].astype(f32) + g.astype(bf16).astype(f32)).astype(bf16)

    outs = [pltpu.make_async_copy(src, dst, out_sem.at[n]) for n, (src, dst) in enumerate(((dh, dmid_h), (gd, gd_h), (gg, gg_h), (gu, gu_h)))]
    for out in outs:
        out.start()
    down.finish(D // DW)
    wide.finish(n)
    for out in outs:
        out.wait()


def ffn_back(dh, b, mid, m, wg, wu, wd, number):
    T, D = dh.shape
    F = m.shape[1]
    shape = lambda r, c: jax.ShapeDtypeStruct((r, c), bf16)
    v = lambda *s: pltpu.VMEM(s, bf16)
    rows, long = D // BLOCKS, F // BLOCKS
    any_ = pl.BlockSpec(memory_space=pl.ANY)
    return pl.pallas_call(
        ffn_back_kernel,
        out_shape=[shape(T, D), shape(long, D), shape(rows, F), shape(rows, F)],
        in_specs=[any_] * 7,
        out_specs=[any_] * 4,
        scratch_shapes=[v(T, D), v(T, D), v(D, T), v(2, T, 640), v(F, T), v(2, D, CHUNK), v(2, D, CHUNK), v(2, CHUNK, D), pltpu.VMEM((T, D), f32),
                        v(T, CHUNK), v(T, CHUNK), v(T, WIDE), v(long, D), v(rows, F), v(rows, F), SEM((2,)), SEM((2,)), SEM((3, 2)), SEM((4,)),
                        *Sums.scratch(long, DW, FFN_LAG, 2 * DW), *Sums.scratch(rows, WIDE, FFN_LAG)],
        compiler_params=params(number),
        name="ffn_back",
    )(dh, b, mid, m, wg, wu, wd)


def stacked(ref, rows, at):
    return jnp.concatenate([ref[rows, at + n * HEAD : at + (n + 1) * HEAD] for n in range(HEADS)], axis=0)


def swapped(t):
    return jnp.concatenate([t[:, HEAD // 2 :], t[:, : HEAD // 2]], axis=1)


def attention_back_kernel(dmid_h, a_h, h_h, qkv_h, att_h, lse_h, cos_h, sin_h, wo_h, wqkv_h, dh_h, go_h, gqkv_h,
                          dmid, a, at, h, qkv, att, att_t, lse, cos, sin, wo, wqkv, datt, delta, dqkv, dq, dk, dv, da, go, gqkv, in_sem, out_sem, *sums):
    T, D = a.shape
    wide = Sums(sums, D // BLOCKS, WIDE, ATT_LAG)
    pairs = ((dmid_h, dmid), (wo_h, wo), (att_h, att), (lse_h, lse), (qkv_h, qkv), (a_h, a), (cos_h, cos), (sin_h, sin), (wqkv_h, wqkv), (h_h, h))
    loads = [pltpu.make_async_copy(src, dst, in_sem.at[n]) for n, (src, dst) in enumerate(pairs)]
    for load in loads:
        load.start()
    wide.greet()
    for load in loads[:3]:
        load.wait()
    att_t[...] = att[...].T

    def term(left, right, n):
        @tiles(D)
        def _(rows):
            wide.term[n % 2, rows, :] = nn(left[rows, :], right)

    def o_item(n):
        cols = slice(n * WIDE, (n + 1) * WIDE)

        def store(total):
            go[:, cols] = total
        return (lambda: term(att_t, dmid[:, cols], n)), wide, n, (n % 2, 0), store

    def from_o():
        @tiles(T)
        def _(rows):
            datt[rows, :] = nt(dmid[rows, :], wo[...]).astype(bf16)

        for n in range(HEADS * GROUPS):
            cols = slice(n * HEAD, (n + 1) * HEAD)
            product = datt[:, cols].astype(f32) * att[:, cols].astype(f32)
            delta[n : n + 1, :] = product.T.sum(0, keepdims=True)
        for load in loads[3:]:
            load.wait()

    def queries(g, iq):
        def run():
            rows = slice(iq * BQ, (iq + 1) * BQ)
            first = g * PART
            q, d_out = stacked(qkv, rows, first), stacked(datt, rows, g * HEADS * HEAD)
            row = lambda ref: jnp.concatenate([ref[g * HEADS + n : g * HEADS + n + 1, rows] for n in range(HEADS)], axis=1)
            bottom, less = row(lse) * LOG2E, row(delta)
            if iq == 0:
                dk[...] = jnp.zeros_like(dk)
                dv[...] = jnp.zeros_like(dv)
            dq[...] = jnp.zeros_like(dq)
            strip = 2 * BQ

            def keys(j, masked):
                here = pl.ds(pl.multiple_of(j * BQ, BQ), BQ)
                k, v = qkv[here, first + V_AT - HEAD : first + V_AT], qkv[here, first + V_AT : first + PART]
                for n in range(0, HEADS * BQ, strip):
                    qs, ds = q[n : n + strip], d_out[n : n + strip]
                    p = jnp.exp2(nt(k, qs) * (SCALE * LOG2E) - bottom[:, n : n + strip])
                    if masked:
                        gap = lax.rem(lax.broadcasted_iota(jnp.int32, p.shape, 1), BQ) - lax.broadcasted_iota(jnp.int32, p.shape, 0)
                        p = jnp.where(gap >= 0, p, 0.0)
                    dp = (p * (nt(v, ds) - less[:, n : n + strip])).astype(bf16)
                    dv[here, :] += nn(p.astype(bf16), ds)
                    dk[here, :] += nn(dp, qs)
                    dq[:, n : n + strip] += tn(k, dp)

            if iq:
                pl.loop(0, iq)(lambda j: keys(j, False))
            keys(iq, True)
            back = lambda t, where: t * cos[where, :] + swapped(t) * -sin[where, :]
            low = lambda t: (t * SCALE).astype(bf16).astype(f32)
            for n in range(HEADS):
                dqkv[rows, first + n * HEAD : first + (n + 1) * HEAD] = back(low(dq[:, n * BQ : (n + 1) * BQ].T), rows).astype(bf16)
            if iq == T // BQ - 1:
                every = slice(0, T)
                dqkv[:, first + V_AT - HEAD : first + V_AT] = back(low(dk[...]), every).astype(bf16)
                dqkv[:, first + V_AT : first + PART] = dv[...].astype(bf16)
        return run

    def qkv_item(g, piece):
        n = D // WIDE + g * (PART // WIDE) + piece
        cols = slice(g * PART + piece * WIDE, g * PART + (piece + 1) * WIDE)

        def run():
            if g == 0 and piece == 0:
                at[...] = a[...].T
            term(at, dqkv[:, cols], n)

        def store(total):
            gqkv[:, cols] = total
        return run, wide, n, (n % 2, 0), store

    def to_a(g):
        def run():
            @tiles(T)
            def _(rows):
                more = nt(dqkv[rows, g * PART : (g + 1) * PART], wqkv[:, g * PART : (g + 1) * PART])
                if g == 0:
                    da[rows, :] = more
                else:
                    g32 = norm_back((da[rows, :] + more).astype(bf16).astype(f32), h[rows, :].astype(f32))
                    dmid[rows, :] = (dmid[rows, :].astype(f32) + g32.astype(bf16).astype(f32)).astype(bf16)
        return run

    items = [o_item(n) for n in range(D // WIDE)] + [(from_o,)]
    for g in range(GROUPS):
        items += [(queries(g, iq),) for iq in range(T // BQ)] + [qkv_item(g, piece) for piece in range(PART // WIDE)] + [(to_a(g),)]
    pipeline(items, ATT_LAG)
    outs = [pltpu.make_async_copy(src, dst, out_sem.at[n]) for n, (src, dst) in enumerate(((dmid, dh_h), (go, go_h), (gqkv, gqkv_h)))]
    for out in outs:
        out.start()
    wide.finish(D // WIDE + GROUPS * PART // WIDE)
    for out in outs:
        out.wait()


def attention_back(dmid, a, h, qkv, att, lse, cos, sin, wo, wqkv, number):
    T, D = a.shape
    P = qkv.shape[1]
    shape = lambda r, c: jax.ShapeDtypeStruct((r, c), bf16)
    v = lambda *s: pltpu.VMEM(s, bf16)
    w = lambda *s: pltpu.VMEM(s, f32)
    any_ = pl.BlockSpec(memory_space=pl.ANY)
    return pl.pallas_call(
        attention_back_kernel,
        out_shape=[shape(T, D), shape(D // BLOCKS, D), shape(D // BLOCKS, P)],
        in_specs=[any_] * 10,
        out_specs=[any_] * 3,
        scratch_shapes=[v(T, D), v(T, D), v(D, T), v(T, D), v(T, P), v(T, D), v(D, T), w(*lse.shape), w(T, HEAD), w(T, HEAD), v(D, D), v(D, P), v(T, D),
                        w(HEADS * GROUPS, T), v(T, P), w(HEAD, HEADS * BQ), w(T, HEAD), w(T, HEAD), w(T, D), v(D // BLOCKS, D), v(D // BLOCKS, P),
                        SEM((10,)), SEM((3,)), *Sums.scratch(D // BLOCKS, WIDE, ATT_LAG)],
        compiler_params=params(number),
        name="attention_back",
    )(dmid, a, h, qkv, att, lse, cos, sin, wo, wqkv)


LAYERS = 2
AHEAD = 2
ALONG = (1, 2, 0)
MATRICES = ("qkv", "o", "gate", "up", "down")
OVER_X = ("qkv", "gate", "up")


class Gather:
    def __init__(self, srcs, outs, own, sems, halves):
        self.srcs, self.outs, self.own, self.halves = srcs, outs, own, halves
        self.load_sem, self.store_sem, self.send_sem, self.c_sem, self.chip_sem, self.x_sem = sems
        self.x, self.y, self.z, self.c = where_am_i()
        self.bits = chip_bits(self.y, self.z)
        n = len(srcs)
        self.items = [(i, l) for l in range(LAYERS) for i in range(n)]
        self.loads = [pltpu.make_async_copy(srcs[i], own[i], self.load_sem.at[i]) for i in range(n)]

    def begin(self):
        for load in self.loads:
            load.start()
        greet([{"c": 1 - self.c}, {"x": 1 - self.x}] + [partner(self.bits, bit) for bit in range(len(self.bits))])
        for load in self.loads:
            load.wait()

    def part(self, ref, item, part):
        half = self.halves[item[0]]
        return ref if half is None or part is None else ref.at[pl.ds(pl.multiple_of(part * half, half), half)]

    def mine(self, item, part):
        i, l = item
        return self.part(self.own[i].at[l], item, part)

    def block(self, item, flips, part):
        i, l = item
        number = 0
        for bit, value in enumerate(self.bits):
            number = number * 2 + ((1 - value) if bit in flips else value)
        return self.part(self.outs[l][i].at[number * 2 + self.c], item, part)

    def remote(self, item, src, dst, sem, **there):
        i, l = item
        return pltpu.make_async_remote_copy(src, dst, self.send_sem.at[l, i], sem, device_id=peer(**there), device_id_type=pl.DeviceIdType.MESH)

    def pass_on(self, item, src, dst, flips, stage):
        i, l = item
        for bit in ALONG[stage:]:
            self.remote(item, src, dst, self.chip_sem.at[l, i, self.index(item, (*flips, bit))], **partner(self.bits, bit)).start()
        if flips:
            if self.halves[i] is not None:
                self.remote(item, src, dst, self.x_sem.at[l, i, self.index(item, flips)], x=1 - self.x).start()
            self.remote(item, src, dst, self.c_sem.at[l, i], c=1 - self.c).start()

    def index(self, item, flips):
        return sum(2**bit for bit in flips) - 1

    def start(self, item):
        i, l = item
        whole = self.block(item, (), None)
        pltpu.make_async_copy(self.own[i].at[l], whole, self.store_sem.at[l, i]).start()
        self.pass_on(item, self.mine(item, self.x), self.block(item, (), self.x), (), 0)
        self.remote(item, self.own[i].at[l], whole, self.c_sem.at[l, i], c=1 - self.c).start()

    def routes(self, item, stage):
        before, bit = ALONG[:stage], ALONG[stage]
        return [(*(b for n, b in enumerate(before) if mask >> n & 1), bit) for mask in range(2**stage)]

    def from_chips(self, item, stage):
        i, l = item
        for flips in self.routes(item, stage):
            ref = self.block(item, flips, self.x)
            self.remote(item, ref, ref, self.chip_sem.at[l, i, self.index(item, flips)], c=1 - self.c).wait_recv()
            self.pass_on(item, ref, ref, flips, stage + 1)

    def from_group(self, item):
        i, l = item
        if self.halves[i] is not None:
            for stage in range(len(self.bits)):
                for flips in self.routes(item, stage):
                    ref = self.block(item, flips, 1 - self.x)
                    self.remote(item, ref, ref, self.x_sem.at[l, i, self.index(item, flips)], c=1 - self.c).wait_recv()
                    self.remote(item, ref, ref, self.c_sem.at[l, i], c=1 - self.c).start()

    def whole(self, item):
        i, l = item
        half = self.outs[l][i].at[pl.ds(0, 8)]
        self.remote(item, half, half, self.c_sem.at[l, i], c=1 - self.c).wait_recv()
        pltpu.make_async_copy(self.own[i].at[l], self.block(item, (), None), self.store_sem.at[l, i]).wait()

    def finish(self):
        for item in self.items:
            i, l = item
            sent = self.outs[l][i].at[pl.ds(0, 15)]
            self.remote(item, sent, sent, self.c_sem.at[l, i], c=1 - self.c).wait_send()

    def steps(self):
        m, bits = len(self.items), len(self.bits)
        out = [(lambda item=item: self.start(item), None) for item in self.items[:AHEAD]]
        for k in range(m + LAGS[bits]):
            for stage, lag in enumerate(LAGS[:bits]):
                if 0 <= k - lag < m:
                    out.append((lambda item=self.items[k - lag], stage=stage: self.from_chips(item, stage), None))
                if stage == 0 and k + AHEAD < m:
                    out.append((lambda item=self.items[k + AHEAD]: self.start(item), None))
            if 0 <= k - LAGS[bits] < m:
                out.append((lambda item=self.items[k - LAGS[bits]]: self.from_group(item), self.items[k - LAGS[bits]]))
        return out


def forward_kernel(*refs, halves):
    n = len(MATRICES)
    take = iter(refs)
    some = lambda count: [next(take) for _ in range(count)]
    srcs, (x_h, cos_h, sin_h) = some(n), some(3)
    outs = [some(n) for _ in range(LAYERS)]
    kept = [some(8) for _ in range(LAYERS)]
    own, sems = some(n), some(6)
    h, cos, sin, wqkv, wo, a, qkv, att, lse, mid, b, m, acc, wg, wu, wd, in_sem, w_sem, out_sem = take
    T, D = h.shape
    F = m.shape[1]
    chunks = [(at, min(CHUNK, F - at)) for at in range(0, F, CHUNK)]
    net = Gather(srcs, outs, own, sems, halves)
    tables = [pltpu.make_async_copy(src, dst, in_sem.at[k]) for k, (src, dst) in enumerate(((x_h, h), (cos_h, cos), (sin_h, sin)))]
    for copy in tables:
        copy.start()
    net.begin()
    pieces = []
    add = lambda l, *need: lambda run: pieces.append(([(MATRICES.index(name), l) for name in need], run))
    flat = lambda l, name: outs[l][MATRICES.index(name)]
    saved = lambda l, k, src: pltpu.make_async_copy(src, kept[l][k], out_sem.at[k])
    flow = dict(enumerate((a, h, qkv, att, lse, mid, b, m)))

    def rows_of(w_h, at, w):
        return w_h.at[:, :, pl.ds(at, w)]

    def w_copies(l, j):
        s, (at, w) = j % 2, chunks[j]
        pairs = ((rows_of(flat(l, "gate"), at, w), wg.at[s, :, :, pl.ds(0, w)]), (rows_of(flat(l, "up"), at, w), wu.at[s, :, :, pl.ds(0, w)]))
        return [pltpu.make_async_copy(src, dst, w_sem.at[k, s]) for k, (src, dst) in enumerate(pairs)]

    def d_copy(l, j):
        return pltpu.make_async_copy(flat(l, "down").at[pl.ds(2 * j, 2)], wd.at[j % 2], w_sem.at[2, j % 2])

    for l in range(LAYERS):
        qkv_in = pltpu.make_async_copy(flat(l, "qkv"), wqkv, in_sem.at[3])
        o_in = pltpu.make_async_copy(flat(l, "o"), wo, in_sem.at[4])

        @add(l, "qkv")
        def _(l=l, qkv_in=qkv_in):
            qkv_in.start()
            if l == 0:
                for copy in tables:
                    copy.wait()
            else:
                saved(0, 0, a).wait()
                saved(0, 2, qkv).wait()
                saved(l, 1, h).start()

        @add(l, "qkv")
        def _(l=l, qkv_in=qkv_in):
            qkv_in.wait()
            w = wqkv[...].reshape(D, GROUPS * PART)

            @tiles(T)
            def _(rows):
                a[rows, :] = norm(h[rows, :].astype(f32))
                for g in range(GROUPS):
                    first = g * PART
                    got = nn(a[rows, :], w[:, first : first + PART]).astype(bf16)
                    for k in range(HEADS + 1):
                        t = got[:, k * HEAD : (k + 1) * HEAD].astype(f32)
                        qkv[rows, first + k * HEAD : first + (k + 1) * HEAD] = (t * cos[rows, :] + swapped(t) * sin[rows, :]).astype(bf16)
                    qkv[rows, first + V_AT : first + PART] = got[:, V_AT:]

            saved(l, 0, a).start()
            saved(l, 2, qkv).start()
            if l:
                saved(0, 3, att).wait()
                saved(0, 4, lse).wait()

        for iq in range(T // BQ):
            @add(l, "qkv")
            def _(iq=iq):
                attend_block(qkv, att, lse, iq)

        @add(l, "o")
        def _(l=l, o_in=o_in):
            o_in.start()
            saved(l, 3, att).start()
            saved(l, 4, lse).start()
            if l:
                saved(0, 5, mid).wait()
                saved(0, 6, b).wait()

        @add(l, "o")
        def _(l=l, o_in=o_in):
            o_in.wait()
            w = wo[...].reshape(D, D)

            @tiles(T)
            def _(rows):
                mid[rows, :] = (h[rows, :].astype(f32) + nn(att[rows, :], w).astype(bf16).astype(f32)).astype(bf16)
                b[rows, :] = norm(mid[rows, :].astype(f32))

            saved(l, 5, mid).start()
            saved(l, 6, b).start()

        @add(l, "gate", "up")
        def _(l=l):
            for copy in w_copies(l, 0):
                copy.start()
            if l:
                saved(0, 7, m).wait()

        for j, (at, w) in enumerate(chunks):
            @add(l, "gate", "up")
            def _(l=l, j=j, at=at, w=w):
                if j + 1 < len(chunks):
                    for copy in w_copies(l, j + 1):
                        copy.start()
                for copy in w_copies(l, j):
                    copy.wait()
                left, right = (t[j % 2, :, :, :w].reshape(D, w) for t in (wg, wu))

                @tiles(T)
                def _(rows):
                    gate, up = nn(b[rows, :], left), nn(b[rows, :], right)
                    m[rows, at : at + w] = (gate * (1 / (1 + jnp.exp(-gate))) * up).astype(bf16)

        @add(l, "gate", "up")
        def _(l=l):
            saved(l, 7, m).start()

        if l + 1 < LAYERS:
            @add(l, "down")
            def _(l=l):
                d_copy(l, 0).start()

            wide = F // 8
            for j in range(8):
                @add(l, "down")
                def _(l=l, j=j):
                    if j < 7:
                        d_copy(l, j + 1).start()
                    d_copy(l, j).wait()
                    w = wd[j % 2].reshape(wide, D)

                    @tiles(T)
                    def _(rows):
                        acc[rows, :] = nn(m[rows, j * wide : (j + 1) * wide], w) + (acc[rows, :] if j else 0.0)

            @add(l, "down")
            def _():
                @tiles(T)
                def _(rows):
                    h[rows, :] = (mid[rows, :].astype(f32) + acc[rows, :].astype(bf16).astype(f32)).astype(bf16)

    arrived, waited = set(), set()

    def ready(need):
        return all(item in arrived for item in need)

    def do_piece():
        need, run = pieces.pop(0)
        for item in need:
            if item not in waited:
                net.whole(item)
                waited.add(item)
        run()

    for run, item in net.steps():
        run()
        if item is not None:
            arrived.add(item)
        for _ in range(PER_STEP):
            if pieces and ready(pieces[0][0]):
                do_piece()
    while pieces:
        do_piece()
    for item in net.items:
        if item not in waited:
            net.whole(item)
    net.finish()
    for k, src in flow.items():
        saved(LAYERS - 1, k, src).wait()


def forward(blocks, x, cos, sin):
    n = len(blocks)
    T, D = x.shape
    rows = D // BLOCKS
    F, P = blocks[2].shape[2], blocks[0].shape[2]
    halves = [b.shape[1] // 2 if name in OVER_X else None for name, b in zip(MATRICES, blocks, strict=True)]
    any_ = pl.BlockSpec(memory_space=pl.ANY)
    v = lambda *s: pltpu.VMEM(s, bf16)
    w = lambda *s: pltpu.VMEM(s, f32)
    shape = lambda *s: jax.ShapeDtypeStruct(s, bf16)
    stats = jax.ShapeDtypeStruct((HEADS * GROUPS, T), f32)
    kept = [shape(T, D), shape(T, D), shape(T, P), shape(T, D), stats, shape(T, D), shape(T, D), shape(T, F)]
    outs = [shape(BLOCKS, *b.shape[1:]) for b in blocks] * LAYERS + kept * LAYERS
    got = pl.pallas_call(
        functools.partial(forward_kernel, halves=halves),
        out_shape=outs,
        in_specs=[any_] * (n + 3),
        out_specs=[any_] * len(outs),
        scratch_shapes=[
            *(pltpu.VMEM(b.shape, bf16) for b in blocks),
            SEM((n,)), *(SEM((LAYERS, n)),) * 3, *(SEM((LAYERS, n, 7)),) * 2,
            v(T, D), w(T, HEAD), w(T, HEAD), v(BLOCKS, rows, P), v(BLOCKS, rows, D), v(T, D), v(T, P), v(T, D), w(*stats.shape), v(T, D), v(T, D), v(T, F), w(T, D),
            *(v(2, BLOCKS, rows, CHUNK),) * 2, v(2, 2, F // BLOCKS, D), SEM((5,)), SEM((3, 2)), SEM((8,)),
        ],
        compiler_params=params(1),
        name="gather_and_forward",
    )(*blocks, x, cos, sin)
    full = [[w.reshape(-1, w.shape[2]) for w in got[l * n : (l + 1) * n]] for l in range(LAYERS)]
    rest = got[LAYERS * n :]
    return full, [list(rest[l * 8 : (l + 1) * 8]) for l in range(LAYERS)]


THETA = 10000


def turns(tokens):
    half = HEAD // 2
    angle = jnp.arange(tokens, dtype=f32)[:, None] * THETA ** (-jnp.arange(half, dtype=f32) / half)
    cos, sin = jnp.cos(angle), jnp.sin(angle)
    return jnp.concatenate([cos, cos], 1), jnp.concatenate([-sin, sin], 1)


def by_key_head(wq, wk, wv):
    q = HEADS * HEAD
    return jnp.concatenate([w[:, :, g * n : (g + 1) * n] for g in range(GROUPS) for w, n in ((wq, q), (wk, HEAD), (wv, HEAD))], axis=2)


def by_kind(t):
    q = HEADS * HEAD
    spans = ((0, q), (q, q + HEAD), (q + HEAD, PART))
    return [jnp.concatenate([t[:, g * PART + a : g * PART + b] for g in range(GROUPS)], axis=1) for a, b in spans]


def solution(mesh):
    fine = jax.sharding.Mesh(mesh.devices.reshape(2, 2, 4, 2), ("x", "y", "z", "c"))

    def step(x, dy, wq, wk, wv, wo, w_gate, w_up, w_down):
        cos, sin = turns(x.shape[1])
        full, saved = forward([by_key_head(wq, wk, wv), wo, w_gate, w_up, w_down], x[0], cos, sin)
        dh, grads = dy[0], []
        for number in reversed(range(LAYERS)):
            pqkv, po, pg, pu, pd = full[number]
            if number == 0:
                saved[number][1] = x[0]
            a, h, qkv, att, lse, mid, b, m = saved[number]
            dmid, *ffn = ffn_back(dh, b, mid, m, pg, pu, pd, 2 + number)
            dh, by_o, by_qkv = attention_back(dmid, a, h, qkv, att, lse, cos, sin, po, pqkv, 2 + LAYERS + number)
            down, gate, up = ffn
            grads.insert(0, (*by_kind(by_qkv), by_o, gate, up, down))
        return (dh[None], *(jnp.stack(same) for same in zip(*grads, strict=True)))

    group = ("y", "z", "c")
    states, cut = P(("x", *group), None, None), P(None, group, None)
    return jax.shard_map(
        step,
        mesh=fine,
        in_specs=(states, states) + (cut,) * 7,
        out_specs=(states,) + (P("x", group, None),) * 7,
        check_vma=False,
    )
```

```python
import functools

import jax
import jax.numpy as jnp
from jax import lax
from jax.experimental import pallas as pl
from jax.experimental.pallas import tpu as pltpu
from jax.sharding import PartitionSpec as P

bf16, f32 = jnp.bfloat16, jnp.float32
SEM = pltpu.SemaphoreType.DMA


def nn(a, b):
    return lax.dot_general(a, b, (((1,), (0,)), ((), ())), preferred_element_type=f32)


def nt(a, b):
    return lax.dot_general(a, b, (((1,), (1,)), ((), ())), preferred_element_type=f32)


def tn(a, b):
    return lax.dot_general(a, b, (((0,), (0,)), ((), ())), preferred_element_type=f32)


def where_am_i():
    return tuple(lax.axis_index(name) for name in ("x", "y", "z", "c"))


def peer(**there):
    at = dict(zip(("x", "y", "z", "c"), where_am_i()), **there)
    return at["x"], at["y"], at["z"], at["c"]


def greet(peers):
    barrier = pltpu.get_barrier_semaphore()
    for there in peers:
        pl.semaphore_signal(barrier, inc=1, device_id=peer(**there), device_id_type=pl.DeviceIdType.MESH)
    pl.semaphore_wait(barrier, len(peers))


def norm_back(g, wide):
    scale = lax.rsqrt(jnp.mean(wide * wide, -1, keepdims=True) + 1e-6)
    return g * scale - wide * (scale * scale * scale * jnp.mean(g * wide, -1, keepdims=True))


HEADS, GROUPS, HEAD = 4, 2, 128
PART = (HEADS + 2) * HEAD
BQ = 256
SCALE = HEAD**-0.5
LOG2E = 1.4426950408889634


PER_STEP = 2
LAGS = (0, 1, 2, 3)
V_AT = (HEADS + 1) * HEAD


def params(number):
    return pltpu.CompilerParams(collective_id=number, has_side_effects=True, vmem_limit_bytes=63 * 2**20)


def tiles(rows, size=512):
    def run(body):
        @pl.loop(0, rows // size)
        def _(t):
            body(pl.ds(pl.multiple_of(t * size, size), size))
    return run


def norm(wide):
    return (wide * lax.rsqrt(jnp.mean(wide * wide, -1, keepdims=True) + 1e-6)).astype(bf16)


def attend_block(qkv, att, lse, iq):
    for g in range(GROUPS):
        rows, seen, first = slice(iq * BQ, (iq + 1) * BQ), (iq + 1) * BQ, g * PART
        k, v = qkv[:seen, first + V_AT - HEAD : first + V_AT], qkv[:seen, first + V_AT : first + PART]
        for n in range(0, HEADS, 2):
            q = jnp.concatenate([qkv[rows, first + i * HEAD : first + (i + 1) * HEAD] for i in (n, n + 1)], axis=0)
            s = nt(k, q)
            gap = lax.rem(lax.broadcasted_iota(jnp.int32, (BQ, 2 * BQ), 1), BQ) - lax.broadcasted_iota(jnp.int32, (BQ, 2 * BQ), 0)
            last = jnp.where(gap >= 0, s[iq * BQ :], -1e30)
            s = jnp.concatenate([s[: iq * BQ], last], axis=0) if iq else last
            top = s.max(0, keepdims=True)
            p = jnp.exp2((s - top) * (SCALE * LOG2E))
            total = p.sum(0, keepdims=True)
            out = tn(v, p.astype(bf16)) * (1 / total)
            stat = top * SCALE + jnp.log(total)
            for i in (0, 1):
                head = g * HEADS + n + i
                att[rows, head * HEAD : (head + 1) * HEAD] = out[:, i * BQ : (i + 1) * BQ].T.astype(bf16)
                lse[head : head + 1, rows] = stat[:, i * BQ : (i + 1) * BQ]


def chip_bits(y, z):
    return [y, lax.div(z, 2), lax.rem(z, 2)]


def partner(bits, bit):
    y, high, low = bits
    return [{"y": 1 - y}, {"z": (1 - high) * 2 + low}, {"z": high * 2 + 1 - low}][bit]


class Sums:
    ORDERS = ((0, 2, 1), (2, 0, 1))
    REFS = 13
    SHARE = 4

    @classmethod
    def places_for(cls, lag):
        return 2 * lag + cls.SHARE - 1

    @classmethod
    def scratch(cls, rows, width, lag, stored=None):
        halves = [(n, size, rows, width) for n, size in zip(lag, (4, 2, 1))]
        return [
            pltpu.VMEM((2, 16 * rows, stored or width), f32),
            *(pltpu.VMEM((2, 8, rows, width), bf16) for _ in range(2)),
            *(pltpu.VMEM(s, f32) for s in halves),
            *(pltpu.VMEM(s, bf16) for s in halves),
            *(pltpu.VMEM((cls.places_for(s[0]), *s[1:]), bf16) for s in halves),
            SEM((4, 2, cls.places_for(max(lag)))),
        ]

    def __init__(self, refs, rows, width, lag):
        self.term, self.c_out, self.c_in, *rest, self.sem = refs
        self.keep, self.out, self.into = rest[:3], rest[3:6], rest[6:]
        self.rows, self.width, self.lag = rows, width, lag
        _, y, z, self.c = where_am_i()
        self.bits = chip_bits(y, z)
        self.count = 0

    def slot(self, i, stage):
        return i % (2 if stage == 0 else self.lag[stage - 1])

    def landing(self, i, stage):
        return i % (2 if stage == 0 else self.places_for(self.lag[stage - 1]))

    def order(self, i):
        return self.ORDERS[1 if i % self.SHARE == self.SHARE - 1 else 0]

    def partner(self, bit):
        return partner(self.bits, bit)

    def greet(self):
        greet([{"c": 1 - self.c}] + [partner(self.bits, bit) for bit in self.ORDERS[0]])

    def copy(self, i, stage):
        s = self.slot(i, stage)
        d = self.landing(i, stage)
        src, dst = (self.c_out, self.c_in) if stage == 0 else (self.out[stage - 1], self.into[stage - 1])
        to = {"c": 1 - self.c} if stage == 0 else self.partner(self.order(i)[stage - 1])
        return pltpu.make_async_remote_copy(src.at[s], dst.at[d], self.sem.at[stage, 0, s], self.sem.at[stage, 1, d],
                                            device_id=peer(**to), device_id_type=pl.DeviceIdType.MESH)

    def block(self, k, c, at):
        slot, column = at
        return self.term[slot, pl.ds(pl.multiple_of((2 * k + c) * self.rows, 8), self.rows), column : column + self.width]

    def to_core(self, i, at):
        if i >= 2:
            self.copy(i - 2, 0).wait_send()

        @pl.loop(0, 8)
        def _(k):
            self.c_out[i % 2, k] = self.block(k, 1 - self.c, at).astype(bf16)

        self.copy(i, 0).start()

    def places(self, i, stage, side):
        order = self.order(i)
        left = sorted(order[stage - 1 :])
        bit = order[stage - 1]
        mine = self.bits[bit]
        want = mine if side == 0 else 1 - mine
        rest = [b for b in left if b != bit]
        out = []
        for n in range(2 ** len(rest)):
            value = {b: (n >> (len(rest) - 1 - j)) & 1 for j, b in enumerate(rest)}
            value[bit] = want
            k = 0
            for b in left:
                k = k * 2 + value[b]
            out.append(k)
        return out

    def to_chip(self, i, stage, at=None):
        s, before, came = self.slot(i, stage), self.slot(i, stage - 1), self.landing(i, stage - 1)
        if i >= self.lag[stage - 1]:
            self.copy(i - self.lag[stage - 1], stage).wait_send()
        self.copy(i, stage - 1).wait_recv()

        def value(k):
            if stage == 1:
                return self.block(k, self.c, at) + self.c_in[came, k].astype(f32)
            return self.keep[stage - 2][before, k] + self.into[stage - 2][came, k].astype(f32)

        for n, k in enumerate(self.places(i, stage, 1)):
            self.out[stage - 1][s, n] = value(k).astype(bf16)
        for n, k in enumerate(self.places(i, stage, 0)):
            self.keep[stage - 1][s, n] = value(k)
        self.copy(i, stage).start()

    def total(self, i):
        self.copy(i, 3).wait_recv()
        return self.keep[2][self.slot(i, 3), 0] + self.into[2][self.landing(i, 3), 0].astype(f32)

    def finish(self, count):
        for stage in range(4):
            for i in range(max(count - (2 if stage == 0 else self.lag[stage - 1]), 0), count):
                self.copy(i, stage).wait_send()


class Pipe:
    def __init__(self):
        self.now, self.due = 0, {}

    def at(self, later, stage, item):
        self.due.setdefault(self.now + later, []).append((stage, item))

    def step(self, compute=lambda: None, *item):
        todo = sorted(self.due.pop(self.now, []), key=lambda one: -one[0])
        for stage, (sums, i, place, store) in todo:
            if stage == len(sums.lag) + 1:
                store(sums.total(i).astype(bf16))
            elif stage > 1:
                sums.to_chip(i, stage)
        compute()
        for stage, (sums, i, place, store) in todo:
            if stage == 1:
                sums.to_chip(i, stage, place)
        if item:
            sums, i, place, store = item
            sums.to_core(i, place)
            later = 1
            for stage, lag in enumerate((*sums.lag, None), 1):
                self.at(later, stage, item)
                later += lag or 0
        self.now += 1

    def drain(self):
        while self.due:
            self.step()


BLOCKS, CHUNK, DW, WIDE = 16, 512, 128, 256
WIDE_LAG, DOWN_LAG = (6, 5, 4), (4, 3, 3)


def ffn_phase(pipe, down, wide, dh, given, weights, results, sems, b, bt, m, mt, wg, wu, wd, db, dgate, dup, ends):
    mid_h, b_h, m_h = given[5:]
    _, _, wg_h, wu_h, wd_h = weights
    gd, gg, gu = results[:3]
    in_sem, m_sem, w_sem = sems
    T, D = b.shape
    F = mt.shape[0]
    chunks = [(at, min(CHUNK, F - at)) for at in range(0, F, CHUNK)]
    MT = m.shape[2]

    def w_copies(j):
        s, (at, w) = j % 2, chunks[j]
        pairs = ((wg_h.at[:, pl.ds(at, w)], wg.at[s, :, pl.ds(0, w)]), (wu_h.at[:, pl.ds(at, w)], wu.at[s, :, pl.ds(0, w)]),
                 (wd_h.at[pl.ds(at, w), :], wd.at[s, pl.ds(0, w), :]))
        return [pltpu.make_async_copy(src, dst, w_sem.at[n, s]) for n, (src, dst) in enumerate(pairs)]

    def m_copy(j):
        return pltpu.make_async_copy(m_h.at[:, pl.ds(j * MT, MT)], m.at[j % 2], m_sem.at[j % 2])

    load_b = pltpu.make_async_copy(b_h, b, in_sem.at[0])
    m_copy(0).start()
    m_copy(1).start()
    load_b.start()
    for copy in w_copies(0):
        copy.start()

    def down_term(i):
        def run():
            if i % 2:
                return
            cols = slice(i * DW, (i + 2) * DW)
            if i == 0:
                for j in range(F // MT):
                    m_copy(j).wait()
                    mt[j * MT : (j + 1) * MT, :] = m[j % 2].T
                    if j + 2 < F // MT:
                        m_copy(j + 2).start()

            @tiles(F, F // 5)
            def _(rows):
                down.term[i // 2 % 2, rows, :] = nn(mt[rows, :], dh[:, cols])
        return run

    def down_store(i):
        def run(total):
            gd[:, i * DW : (i + 1) * DW] = total
        return run

    def chunk(j):
        s, (at, w) = j % 2, chunks[j]
        if j == 0:
            load_b.wait()
            bt[...] = b[...].T
        if j + 1 < len(chunks):
            for copy in w_copies(j + 1):
                copy.start()
        for copy in w_copies(j):
            copy.wait()

        @tiles(T)
        def _(rows):
            dm = nt(dh[rows, :], wd[s, :w, :]).astype(bf16).astype(f32)
            gate, up = nn(b[rows, :], wg[s, :, :w]), nn(b[rows, :], wu[s, :, :w])
            sig = 1 / (1 + jnp.exp(-gate))
            to_up = (dm * (gate * sig)).astype(bf16)
            to_gate = (dm * up * (sig * (1 + gate * (1 - sig)))).astype(bf16)
            if w == CHUNK:
                dup[rows, :] = to_up
                dgate[rows, :] = to_gate
            else:
                ends[rows, :w] = to_gate
                ends[rows, w:] = to_up
            term = nt(to_gate, wg[s, :, :w]) + nt(to_up, wu[s, :, :w])
            if j == 0:
                db[rows, :] = term
            else:
                db[rows, :] += term

    def wide_term(j, which, piece, n):
        def run():
            if which == 0 and piece == 0:
                chunk(j)
            right = ends[...] if chunks[j][1] < CHUNK else (dgate, dup)[which][:, piece * WIDE : (piece + 1) * WIDE]

            @tiles(D)
            def _(rows):
                wide.term[n % 2, rows, :] = nn(bt[rows, :], right)
        return run

    def wide_store(j, which, piece):
        at, w = chunks[j]

        def run(total):
            if w < CHUNK:
                gg[:, at : at + w] = total[:, :w]
                gu[:, at : at + w] = total[:, w:]
            else:
                (gg, gu)[which][:, at + piece * WIDE : at + (piece + 1) * WIDE] = total
        return run

    for i in range(D // DW):
        pipe.step(down_term(i), down, i, (i // 2 % 2, i % 2 * DW), down_store(i))
    for j, (at, w) in enumerate(chunks):
        for which, piece in [(which, piece) for which in (0, 1) for piece in range(CHUNK // WIDE)] if w == CHUNK else [(0, 0)]:
            n = wide.count
            wide.count += 1
            pipe.step(wide_term(j, which, piece, n), wide, n, (n % 2, 0), wide_store(j, which, piece))
    mid = b
    load_mid = pltpu.make_async_copy(mid_h, mid, in_sem.at[0])
    load_mid.start()
    load_mid.wait()

    @tiles(T)
    def _(rows):
        g = norm_back(db[rows, :].astype(bf16).astype(f32), mid[rows, :].astype(f32))
        dh[rows, :] = (dh[rows, :].astype(f32) + g.astype(bf16).astype(f32)).astype(bf16)


def stacked(ref, rows, at):
    return jnp.concatenate([ref[rows, at + n * HEAD : at + (n + 1) * HEAD] for n in range(HEADS)], axis=0)


def swapped(t):
    return jnp.concatenate([t[:, HEAD // 2 :], t[:, : HEAD // 2]], axis=1)


def attention_phase(pipe, wide, dmid, given, weights, tables, results, in_sem, a, at, h, qkv, att, att_t, lse, cos, sin, wo, wqkv, delta, dq, dk, dv, da):
    a_h, h_h, qkv_h, att_h, lse_h = given[:5]
    wqkv_h, wo_h = weights[:2]
    go, gqkv = results[3:]
    T, D = a.shape
    datt, dqkv = a, qkv
    pairs = ((att_h, att), (a_h, a), (wo_h, wo), (lse_h, lse), (qkv_h, qkv), (tables[0], cos), (tables[1], sin), (wqkv_h, wqkv), (h_h, h))
    loads = [pltpu.make_async_copy(src, dst, in_sem.at[n]) for n, (src, dst) in enumerate(pairs)]
    for load in loads:
        load.start()
    for load in loads[:3]:
        load.wait()
    att_t[...] = att[...].T
    at[...] = a[...].T

    def term(left, right, n):
        @tiles(D)
        def _(rows):
            wide.term[n % 2, rows, :] = nn(left[rows, :], right)

    def o_item(piece):
        n = wide.count
        wide.count += 1
        cols = slice(piece * WIDE, (piece + 1) * WIDE)

        def store(total):
            go[:, cols] = total
        return (lambda: term(att_t, dmid[:, cols], n)), wide, n, (n % 2, 0), store

    def from_o():
        @tiles(T)
        def _(rows):
            datt[rows, :] = nt(dmid[rows, :], wo[...]).astype(bf16)

        for n in range(HEADS * GROUPS):
            cols = slice(n * HEAD, (n + 1) * HEAD)
            product = datt[:, cols].astype(f32) * att[:, cols].astype(f32)
            delta[n : n + 1, :] = product.T.sum(0, keepdims=True)
        for load in loads[3:]:
            load.wait()

    def queries(g, iq):
        def run():
            rows = slice(iq * BQ, (iq + 1) * BQ)
            first = g * PART
            q, d_out = stacked(qkv, rows, first), stacked(datt, rows, g * HEADS * HEAD)
            row = lambda ref: jnp.concatenate([ref[g * HEADS + n : g * HEADS + n + 1, rows] for n in range(HEADS)], axis=1)
            bottom, less = row(lse) * LOG2E, row(delta)
            if iq == 0:
                dk[...] = jnp.zeros_like(dk)
                dv[...] = jnp.zeros_like(dv)
            dq[...] = jnp.zeros_like(dq)
            strip = 2 * BQ

            def keys(j, masked):
                here = pl.ds(pl.multiple_of(j * BQ, BQ), BQ)
                k, v = qkv[here, first + V_AT - HEAD : first + V_AT], qkv[here, first + V_AT : first + PART]
                for n in range(0, HEADS * BQ, strip):
                    qs, ds = q[n : n + strip], d_out[n : n + strip]
                    p = jnp.exp2(nt(k, qs) * (SCALE * LOG2E) - bottom[:, n : n + strip])
                    if masked:
                        gap = lax.rem(lax.broadcasted_iota(jnp.int32, p.shape, 1), BQ) - lax.broadcasted_iota(jnp.int32, p.shape, 0)
                        p = jnp.where(gap >= 0, p, 0.0)
                    dp = (p * (nt(v, ds) - less[:, n : n + strip])).astype(bf16)
                    dv[here, :] += nn(p.astype(bf16), ds)
                    dk[here, :] += nn(dp, qs)
                    dq[:, n : n + strip] += tn(k, dp)

            if iq:
                pl.loop(0, iq)(lambda j: keys(j, False))
            keys(iq, True)
            back = lambda t, where: t * cos[where, :] + swapped(t) * -sin[where, :]
            low = lambda t: (t * SCALE).astype(bf16).astype(f32)
            for n in range(HEADS):
                dqkv[rows, first + n * HEAD : first + (n + 1) * HEAD] = back(low(dq[:, n * BQ : (n + 1) * BQ].T), rows).astype(bf16)
            if iq == T // BQ - 1:
                every = slice(0, T)
                dqkv[:, first + V_AT - HEAD : first + V_AT] = back(low(dk[...]), every).astype(bf16)
                dqkv[:, first + V_AT : first + PART] = dv[...].astype(bf16)
        return run

    def qkv_item(g, piece):
        n = wide.count
        wide.count += 1
        cols = slice(g * PART + piece * WIDE, g * PART + (piece + 1) * WIDE)

        def run():
            term(at, dqkv[:, cols], n)

        def store(total):
            gqkv[:, cols] = total
        return run, wide, n, (n % 2, 0), store

    def to_a(g):
        def run():
            @tiles(T)
            def _(rows):
                more = nt(dqkv[rows, g * PART : (g + 1) * PART], wqkv[:, g * PART : (g + 1) * PART])
                if g == 0:
                    da[rows, :] = more
                else:
                    g32 = norm_back((da[rows, :] + more).astype(bf16).astype(f32), h[rows, :].astype(f32))
                    dmid[rows, :] = (dmid[rows, :].astype(f32) + g32.astype(bf16).astype(f32)).astype(bf16)
        return run

    for piece in range(D // WIDE):
        pipe.step(*o_item(piece))
    pipe.step(from_o)
    for g in range(GROUPS):
        for iq in range(T // BQ):
            pipe.step(queries(g, iq))
        for piece in range(PART // WIDE):
            pipe.step(*qkv_item(g, piece))
        pipe.step(to_a(g))


def backward_kernel(*refs):
    take = iter(refs)
    some = lambda count: [next(take) for _ in range(count)]
    dy_h, *tables = some(3)
    given, weights = some(8), some(5)
    dx_h, *outs = some(6)
    dh = next(take)
    results = some(5)
    *sems, out_sem = some(4)
    T, D = dh.shape
    F = given[-1].shape[1]
    down, wide = Sums(some(Sums.REFS), F // BLOCKS, DW, DOWN_LAG), Sums(some(Sums.REFS), D // BLOCKS, WIDE, WIDE_LAG)
    load = pltpu.make_async_copy(dy_h, dh, out_sem.at[0])
    load.start()
    down.greet()
    load.wait()
    pipe = Pipe()
    v = lambda *s: pltpu.VMEM(s, bf16)
    w = lambda *s: pltpu.VMEM(s, f32)
    two = lambda *s: v(2, *s)
    pl.run_scoped(
        functools.partial(ffn_phase, pipe, down, wide, dh, given, weights, results, sems),
        v(T, D), v(D, T), two(T, HEAD), v(F, T), two(D, CHUNK), two(D, CHUNK), two(CHUNK, D), w(T, D), v(T, CHUNK), v(T, CHUNK), v(T, WIDE),
    )
    pl.run_scoped(
        functools.partial(attention_phase, pipe, wide, dh, given, weights, tables, results, sems[0]),
        v(T, D), v(D, T), v(T, D), v(*given[2].shape), v(T, D), v(D, T), w(HEADS * GROUPS, T), w(T, HEAD), w(T, HEAD), v(D, D),
        v(*weights[0].shape), w(HEADS * GROUPS, T), w(HEAD, HEADS * BQ), w(T, HEAD), w(T, HEAD), w(T, D),
    )
    out = pltpu.make_async_copy(dh, dx_h, out_sem.at[0])
    out.start()
    pipe.drain()
    copies = [pltpu.make_async_copy(src, dst, out_sem.at[n]) for n, (src, dst) in enumerate(zip(results, outs, strict=True), 1)]
    for copy in copies:
        copy.start()
    down.finish(D // DW)
    wide.finish(wide.count)
    for copy in [out, *copies]:
        copy.wait()


def backward(dy, cos, sin, saved, full, number):
    T, D = dy.shape
    F, P = saved[-1].shape[1], saved[2].shape[1]
    rows, long = D // BLOCKS, F // BLOCKS
    any_ = pl.BlockSpec(memory_space=pl.ANY)
    shapes = [(T, D), (long, D), (rows, F), (rows, F), (rows, D), (rows, P)]
    given = [dy, cos, sin, *saved, *full]
    return pl.pallas_call(
        backward_kernel,
        out_shape=[jax.ShapeDtypeStruct(s, bf16) for s in shapes],
        in_specs=[any_] * len(given),
        out_specs=[any_] * len(shapes),
        scratch_shapes=[*(pltpu.VMEM(s, bf16) for s in shapes), SEM((9,)), SEM((2,)), SEM((3, 2)), SEM((len(shapes),)),
                        *Sums.scratch(long, DW, DOWN_LAG, 2 * DW), *Sums.scratch(rows, WIDE, WIDE_LAG)],
        compiler_params=params(number),
        name="backward",
    )(*given)


LAYERS = 2
AHEAD = 2
ALONG = (1, 2, 0)
MATRICES = ("qkv", "o", "gate", "up", "down")
OVER_X = ("qkv", "gate", "up")


class Gather:
    def __init__(self, srcs, outs, own, sems, halves):
        self.srcs, self.outs, self.own, self.halves = srcs, outs, own, halves
        self.load_sem, self.store_sem, self.send_sem, self.c_sem, self.chip_sem, self.x_sem = sems
        self.x, self.y, self.z, self.c = where_am_i()
        self.bits = chip_bits(self.y, self.z)
        n = len(srcs)
        self.items = [(i, l) for l in range(LAYERS) for i in range(n)]
        self.loads = [pltpu.make_async_copy(srcs[i], own[i], self.load_sem.at[i]) for i in range(n)]

    def begin(self):
        for load in self.loads:
            load.start()
        greet([{"c": 1 - self.c}, {"x": 1 - self.x}] + [partner(self.bits, bit) for bit in range(len(self.bits))])
        for load in self.loads:
            load.wait()

    def part(self, ref, item, part):
        half = self.halves[item[0]]
        return ref if half is None or part is None else ref.at[pl.ds(pl.multiple_of(part * half, half), half)]

    def mine(self, item, part):
        i, l = item
        return self.part(self.own[i].at[l], item, part)

    def block(self, item, flips, part):
        i, l = item
        number = 0
        for bit, value in enumerate(self.bits):
            number = number * 2 + ((1 - value) if bit in flips else value)
        return self.part(self.outs[l][i].at[number * 2 + self.c], item, part)

    def remote(self, item, src, dst, sem, **there):
        i, l = item
        return pltpu.make_async_remote_copy(src, dst, self.send_sem.at[l, i], sem, device_id=peer(**there), device_id_type=pl.DeviceIdType.MESH)

    def pass_on(self, item, src, dst, flips, stage):
        i, l = item
        for bit in ALONG[stage:]:
            self.remote(item, src, dst, self.chip_sem.at[l, i, self.index(item, (*flips, bit))], **partner(self.bits, bit)).start()
        if flips:
            if self.halves[i] is not None:
                self.remote(item, src, dst, self.x_sem.at[l, i, self.index(item, flips)], x=1 - self.x).start()
            self.remote(item, src, dst, self.c_sem.at[l, i], c=1 - self.c).start()

    def index(self, item, flips):
        return sum(2**bit for bit in flips) - 1

    def start(self, item):
        i, l = item
        whole = self.block(item, (), None)
        pltpu.make_async_copy(self.own[i].at[l], whole, self.store_sem.at[l, i]).start()
        self.pass_on(item, self.mine(item, self.x), self.block(item, (), self.x), (), 0)
        self.remote(item, self.own[i].at[l], whole, self.c_sem.at[l, i], c=1 - self.c).start()

    def routes(self, item, stage):
        before, bit = ALONG[:stage], ALONG[stage]
        return [(*(b for n, b in enumerate(before) if mask >> n & 1), bit) for mask in range(2**stage)]

    def from_chips(self, item, stage):
        i, l = item
        for flips in self.routes(item, stage):
            ref = self.block(item, flips, self.x)
            self.remote(item, ref, ref, self.chip_sem.at[l, i, self.index(item, flips)], c=1 - self.c).wait_recv()
            self.pass_on(item, ref, ref, flips, stage + 1)

    def from_group(self, item):
        i, l = item
        if self.halves[i] is not None:
            for stage in range(len(self.bits)):
                for flips in self.routes(item, stage):
                    ref = self.block(item, flips, 1 - self.x)
                    self.remote(item, ref, ref, self.x_sem.at[l, i, self.index(item, flips)], c=1 - self.c).wait_recv()
                    self.remote(item, ref, ref, self.c_sem.at[l, i], c=1 - self.c).start()

    def whole(self, item):
        i, l = item
        half = self.outs[l][i].at[pl.ds(0, 8)]
        self.remote(item, half, half, self.c_sem.at[l, i], c=1 - self.c).wait_recv()
        pltpu.make_async_copy(self.own[i].at[l], self.block(item, (), None), self.store_sem.at[l, i]).wait()

    def finish(self):
        for item in self.items:
            i, l = item
            sent = self.outs[l][i].at[pl.ds(0, 15)]
            self.remote(item, sent, sent, self.c_sem.at[l, i], c=1 - self.c).wait_send()

    def steps(self):
        m, bits = len(self.items), len(self.bits)
        out = [(lambda item=item: self.start(item), None) for item in self.items[:AHEAD]]
        for k in range(m + LAGS[bits]):
            for stage, lag in enumerate(LAGS[:bits]):
                if 0 <= k - lag < m:
                    out.append((lambda item=self.items[k - lag], stage=stage: self.from_chips(item, stage), None))
                if stage == 0 and k + AHEAD < m:
                    out.append((lambda item=self.items[k + AHEAD]: self.start(item), None))
            if 0 <= k - LAGS[bits] < m:
                out.append((lambda item=self.items[k - LAGS[bits]]: self.from_group(item), self.items[k - LAGS[bits]]))
        return out


def forward_kernel(*refs, halves):
    n = len(MATRICES)
    take = iter(refs)
    some = lambda count: [next(take) for _ in range(count)]
    srcs, (x_h, cos_h, sin_h) = some(n), some(3)
    outs = [some(n) for _ in range(LAYERS)]
    kept = [some(8) for _ in range(LAYERS)]
    own, sems = some(n), some(6)
    h, cos, sin, wqkv, wo, a, qkv, att, lse, mid, b, m, acc, wg, wu, wd, in_sem, w_sem, out_sem = take
    T, D = h.shape
    F = m.shape[1]
    chunks = [(at, min(CHUNK, F - at)) for at in range(0, F, CHUNK)]
    net = Gather(srcs, outs, own, sems, halves)
    tables = [pltpu.make_async_copy(src, dst, in_sem.at[k]) for k, (src, dst) in enumerate(((x_h, h), (cos_h, cos), (sin_h, sin)))]
    for copy in tables:
        copy.start()
    net.begin()
    pieces = []
    add = lambda l, *need: lambda run: pieces.append(([(MATRICES.index(name), l) for name in need], run))
    flat = lambda l, name: outs[l][MATRICES.index(name)]
    saved = lambda l, k, src: pltpu.make_async_copy(src, kept[l][k], out_sem.at[k])
    flow = dict(enumerate((a, h, qkv, att, lse, mid, b, m)))

    def rows_of(w_h, at, w):
        return w_h.at[:, :, pl.ds(at, w)]

    def w_copies(l, j):
        s, (at, w) = j % 2, chunks[j]
        pairs = ((rows_of(flat(l, "gate"), at, w), wg.at[s, :, :, pl.ds(0, w)]), (rows_of(flat(l, "up"), at, w), wu.at[s, :, :, pl.ds(0, w)]))
        return [pltpu.make_async_copy(src, dst, w_sem.at[k, s]) for k, (src, dst) in enumerate(pairs)]

    def d_copy(l, j):
        return pltpu.make_async_copy(flat(l, "down").at[pl.ds(2 * j, 2)], wd.at[j % 2], w_sem.at[2, j % 2])

    for l in range(LAYERS):
        qkv_in = pltpu.make_async_copy(flat(l, "qkv"), wqkv, in_sem.at[3])
        o_in = pltpu.make_async_copy(flat(l, "o"), wo, in_sem.at[4])

        @add(l, "qkv")
        def _(l=l, qkv_in=qkv_in):
            qkv_in.start()
            if l == 0:
                for copy in tables:
                    copy.wait()
            else:
                saved(0, 0, a).wait()
                saved(0, 2, qkv).wait()
                saved(l, 1, h).start()

        @add(l, "qkv")
        def _(l=l, qkv_in=qkv_in):
            qkv_in.wait()
            w = wqkv[...].reshape(D, GROUPS * PART)

            @tiles(T)
            def _(rows):
                a[rows, :] = norm(h[rows, :].astype(f32))
                for g in range(GROUPS):
                    first = g * PART
                    got = nn(a[rows, :], w[:, first : first + PART]).astype(bf16)
                    for k in range(HEADS + 1):
                        t = got[:, k * HEAD : (k + 1) * HEAD].astype(f32)
                        qkv[rows, first + k * HEAD : first + (k + 1) * HEAD] = (t * cos[rows, :] + swapped(t) * sin[rows, :]).astype(bf16)
                    qkv[rows, first + V_AT : first + PART] = got[:, V_AT:]

            saved(l, 0, a).start()
            saved(l, 2, qkv).start()
            if l:
                saved(0, 3, att).wait()
                saved(0, 4, lse).wait()

        for iq in range(T // BQ):
            @add(l, "qkv")
            def _(iq=iq):
                attend_block(qkv, att, lse, iq)

        @add(l, "o")
        def _(l=l, o_in=o_in):
            o_in.start()
            saved(l, 3, att).start()
            saved(l, 4, lse).start()
            if l:
                saved(0, 5, mid).wait()
                saved(0, 6, b).wait()

        @add(l, "o")
        def _(l=l, o_in=o_in):
            o_in.wait()
            w = wo[...].reshape(D, D)

            @tiles(T)
            def _(rows):
                mid[rows, :] = (h[rows, :].astype(f32) + nn(att[rows, :], w).astype(bf16).astype(f32)).astype(bf16)
                b[rows, :] = norm(mid[rows, :].astype(f32))

            saved(l, 5, mid).start()
            saved(l, 6, b).start()

        @add(l, "gate", "up")
        def _(l=l):
            for copy in w_copies(l, 0):
                copy.start()
            if l:
                saved(0, 7, m).wait()

        for j, (at, w) in enumerate(chunks):
            @add(l, "gate", "up")
            def _(l=l, j=j, at=at, w=w):
                if j + 1 < len(chunks):
                    for copy in w_copies(l, j + 1):
                        copy.start()
                for copy in w_copies(l, j):
                    copy.wait()
                left, right = (t[j % 2, :, :, :w].reshape(D, w) for t in (wg, wu))

                @tiles(T)
                def _(rows):
                    gate, up = nn(b[rows, :], left), nn(b[rows, :], right)
                    m[rows, at : at + w] = (gate * (1 / (1 + jnp.exp(-gate))) * up).astype(bf16)

        @add(l, "gate", "up")
        def _(l=l):
            saved(l, 7, m).start()

        if l + 1 < LAYERS:
            @add(l, "down")
            def _(l=l):
                d_copy(l, 0).start()

            wide = F // 8
            for j in range(8):
                @add(l, "down")
                def _(l=l, j=j):
                    if j < 7:
                        d_copy(l, j + 1).start()
                    d_copy(l, j).wait()
                    w = wd[j % 2].reshape(wide, D)

                    @tiles(T)
                    def _(rows):
                        acc[rows, :] = nn(m[rows, j * wide : (j + 1) * wide], w) + (acc[rows, :] if j else 0.0)

            @add(l, "down")
            def _():
                @tiles(T)
                def _(rows):
                    h[rows, :] = (mid[rows, :].astype(f32) + acc[rows, :].astype(bf16).astype(f32)).astype(bf16)

    arrived, waited = set(), set()

    def ready(need):
        return all(item in arrived for item in need)

    def do_piece():
        need, run = pieces.pop(0)
        for item in need:
            if item not in waited:
                net.whole(item)
                waited.add(item)
        run()

    for run, item in net.steps():
        run()
        if item is not None:
            arrived.add(item)
        for _ in range(PER_STEP):
            if pieces and ready(pieces[0][0]):
                do_piece()
    while pieces:
        do_piece()
    for item in net.items:
        if item not in waited:
            net.whole(item)
    net.finish()
    for k, src in flow.items():
        saved(LAYERS - 1, k, src).wait()


def forward(blocks, x, cos, sin):
    n = len(blocks)
    T, D = x.shape
    rows = D // BLOCKS
    F, P = blocks[2].shape[2], blocks[0].shape[2]
    halves = [b.shape[1] // 2 if name in OVER_X else None for name, b in zip(MATRICES, blocks, strict=True)]
    any_ = pl.BlockSpec(memory_space=pl.ANY)
    v = lambda *s: pltpu.VMEM(s, bf16)
    w = lambda *s: pltpu.VMEM(s, f32)
    shape = lambda *s: jax.ShapeDtypeStruct(s, bf16)
    stats = jax.ShapeDtypeStruct((HEADS * GROUPS, T), f32)
    kept = [shape(T, D), shape(T, D), shape(T, P), shape(T, D), stats, shape(T, D), shape(T, D), shape(T, F)]
    outs = [shape(BLOCKS, *b.shape[1:]) for b in blocks] * LAYERS + kept * LAYERS
    got = pl.pallas_call(
        functools.partial(forward_kernel, halves=halves),
        out_shape=outs,
        in_specs=[any_] * (n + 3),
        out_specs=[any_] * len(outs),
        scratch_shapes=[
            *(pltpu.VMEM(b.shape, bf16) for b in blocks),
            SEM((n,)), *(SEM((LAYERS, n)),) * 3, *(SEM((LAYERS, n, 7)),) * 2,
            v(T, D), w(T, HEAD), w(T, HEAD), v(BLOCKS, rows, P), v(BLOCKS, rows, D), v(T, D), v(T, P), v(T, D), w(*stats.shape), v(T, D), v(T, D), v(T, F), w(T, D),
            *(v(2, BLOCKS, rows, CHUNK),) * 2, v(2, 2, F // BLOCKS, D), SEM((5,)), SEM((3, 2)), SEM((8,)),
        ],
        compiler_params=params(1),
        name="gather_and_forward",
    )(*blocks, x, cos, sin)
    full = [[w.reshape(-1, w.shape[2]) for w in got[l * n : (l + 1) * n]] for l in range(LAYERS)]
    rest = got[LAYERS * n :]
    return full, [list(rest[l * 8 : (l + 1) * 8]) for l in range(LAYERS)]


THETA = 10000


def turns(tokens):
    half = HEAD // 2
    angle = jnp.arange(tokens, dtype=f32)[:, None] * THETA ** (-jnp.arange(half, dtype=f32) / half)
    cos, sin = jnp.cos(angle), jnp.sin(angle)
    return jnp.concatenate([cos, cos], 1), jnp.concatenate([-sin, sin], 1)


def by_key_head(wq, wk, wv):
    q = HEADS * HEAD
    return jnp.concatenate([w[:, :, g * n : (g + 1) * n] for g in range(GROUPS) for w, n in ((wq, q), (wk, HEAD), (wv, HEAD))], axis=2)


def by_kind(t):
    q = HEADS * HEAD
    spans = ((0, q), (q, q + HEAD), (q + HEAD, PART))
    return [jnp.concatenate([t[:, g * PART + a : g * PART + b] for g in range(GROUPS)], axis=1) for a, b in spans]


def solution(mesh):
    fine = jax.sharding.Mesh(mesh.devices.reshape(2, 2, 4, 2), ("x", "y", "z", "c"))

    def step(x, dy, wq, wk, wv, wo, w_gate, w_up, w_down):
        cos, sin = turns(x.shape[1])
        full, saved = forward([by_key_head(wq, wk, wv), wo, w_gate, w_up, w_down], x[0], cos, sin)
        saved[0][1] = x[0]
        dh, grads = dy[0], []
        for number in reversed(range(LAYERS)):
            dh, down, gate, up, by_o, by_qkv = backward(dh, cos, sin, saved[number], full[number], 2 + number)
            grads.insert(0, (*by_kind(by_qkv), by_o, gate, up, down))
        return (dh[None], *(jnp.stack(same) for same in zip(*grads, strict=True)))

    group = ("y", "z", "c")
    states, cut = P(("x", *group), None, None), P(None, group, None)
    return jax.shard_map(
        step,
        mesh=fine,
        in_specs=(states, states) + (cut,) * 7,
        out_specs=(states,) + (P("x", group, None),) * 7,
        check_vma=False,
    )
```

```python
import functools

import jax
import jax.numpy as jnp
import numpy as np
from jax import lax
from jax.experimental import pallas as pl
from jax.experimental.pallas import tpu as pltpu
from jax.sharding import PartitionSpec as P

bf16, f32 = jnp.bfloat16, jnp.float32
SEM = pltpu.SemaphoreType.DMA


def nn(a, b):
    return lax.dot_general(a, b, (((1,), (0,)), ((), ())), preferred_element_type=f32)


def nt(a, b):
    return lax.dot_general(a, b, (((1,), (1,)), ((), ())), preferred_element_type=f32)


def tn(a, b):
    return lax.dot_general(a, b, (((0,), (0,)), ((), ())), preferred_element_type=f32)


def where_am_i():
    return tuple(lax.axis_index(name) for name in ("x", "y", "z", "c"))


def peer(**there):
    at = dict(zip(("x", "y", "z", "c"), where_am_i()), **there)
    return at["x"], at["y"], at["z"], at["c"]


def greet(peers):
    barrier = pltpu.get_barrier_semaphore()
    for there in peers:
        pl.semaphore_signal(barrier, inc=1, device_id=peer(**there), device_id_type=pl.DeviceIdType.MESH)
    pl.semaphore_wait(barrier, len(peers))


def norm_back(g, wide):
    scale = lax.rsqrt(jnp.mean(wide * wide, -1, keepdims=True) + 1e-6)
    return g * scale - wide * (scale * scale * scale * jnp.mean(g * wide, -1, keepdims=True))


HEADS, GROUPS, HEAD = 4, 2, 128
PART = (HEADS + 2) * HEAD
BQ = 256
SCALE = HEAD**-0.5
LOG2E = 1.4426950408889634


PER_STEP = 2
LAGS = (0, 1, 2, 3)
V_AT = (HEADS + 1) * HEAD


def params(number):
    return pltpu.CompilerParams(collective_id=number, has_side_effects=True, vmem_limit_bytes=63 * 2**20)


def tiles(rows, size=512):
    def run(body):
        @pl.loop(0, rows // size)
        def _(t):
            body(pl.ds(pl.multiple_of(t * size, size), size))
    return run


def norm(wide):
    return (wide * lax.rsqrt(jnp.mean(wide * wide, -1, keepdims=True) + 1e-6)).astype(bf16)


def attend_block(qkv, att, lse, iq):
    for g in range(GROUPS):
        rows, seen, first = slice(iq * BQ, (iq + 1) * BQ), (iq + 1) * BQ, g * PART
        k, v = qkv[:seen, first + V_AT - HEAD : first + V_AT], qkv[:seen, first + V_AT : first + PART]
        for n in range(0, HEADS, 2):
            q = jnp.concatenate([qkv[rows, first + i * HEAD : first + (i + 1) * HEAD] for i in (n, n + 1)], axis=0)
            s = nt(k, q)
            gap = lax.rem(lax.broadcasted_iota(jnp.int32, (BQ, 2 * BQ), 1), BQ) - lax.broadcasted_iota(jnp.int32, (BQ, 2 * BQ), 0)
            last = jnp.where(gap >= 0, s[iq * BQ :], -1e30)
            s = jnp.concatenate([s[: iq * BQ], last], axis=0) if iq else last
            top = s.max(0, keepdims=True)
            p = jnp.exp2((s - top) * (SCALE * LOG2E))
            total = p.sum(0, keepdims=True)
            out = tn(v, p.astype(bf16)) * (1 / total)
            stat = top * SCALE + jnp.log(total)
            for i in (0, 1):
                head = g * HEADS + n + i
                att[rows, head * HEAD : (head + 1) * HEAD] = out[:, i * BQ : (i + 1) * BQ].T.astype(bf16)
                lse[head : head + 1, rows] = stat[:, i * BQ : (i + 1) * BQ]


def chip_bits(y, z):
    return [y, lax.div(z, 2), lax.rem(z, 2)]


def partner(bits, bit):
    y, high, low = bits
    return [{"y": 1 - y}, {"z": (1 - high) * 2 + low}, {"z": high * 2 + 1 - low}][bit]


class Sums:
    ORDERS = ((0, 2, 1), (2, 0, 1))
    REFS = 13
    SHARE = 4

    @classmethod
    def places_for(cls, lag):
        return 2 * lag + cls.SHARE - 1

    @classmethod
    def scratch(cls, rows, width, lag, stored=None):
        halves = [(n, size, rows, width) for n, size in zip(lag, (4, 2, 1))]
        return [
            pltpu.VMEM((2, 16 * rows, stored or width), f32),
            *(pltpu.VMEM((2, 8, rows, width), bf16) for _ in range(2)),
            *(pltpu.VMEM(s, f32) for s in halves),
            *(pltpu.VMEM(s, bf16) for s in halves),
            *(pltpu.VMEM((cls.places_for(s[0]), *s[1:]), bf16) for s in halves),
            SEM((4, 2, cls.places_for(max(lag)))),
        ]

    def __init__(self, refs, rows, width, lag):
        self.term, self.c_out, self.c_in, *rest, self.sem = refs
        self.keep, self.out, self.into = rest[:3], rest[3:6], rest[6:]
        self.rows, self.width, self.lag = rows, width, lag
        _, y, z, self.c = where_am_i()
        self.bits = chip_bits(y, z)
        self.count = 0

    def slot(self, i, stage):
        return i % (2 if stage == 0 else self.lag[stage - 1])

    def landing(self, i, stage):
        return i % (2 if stage == 0 else self.places_for(self.lag[stage - 1]))

    def order(self, i):
        return self.ORDERS[1 if i % self.SHARE == self.SHARE - 1 else 0]

    def partner(self, bit):
        return partner(self.bits, bit)

    def greet(self):
        greet([{"c": 1 - self.c}] + [partner(self.bits, bit) for bit in self.ORDERS[0]])

    def copy(self, i, stage):
        s = self.slot(i, stage)
        d = self.landing(i, stage)
        src, dst = (self.c_out, self.c_in) if stage == 0 else (self.out[stage - 1], self.into[stage - 1])
        to = {"c": 1 - self.c} if stage == 0 else self.partner(self.order(i)[stage - 1])
        return pltpu.make_async_remote_copy(src.at[s], dst.at[d], self.sem.at[stage, 0, s], self.sem.at[stage, 1, d],
                                            device_id=peer(**to), device_id_type=pl.DeviceIdType.MESH)

    def block(self, k, c, at):
        slot, column = at
        return self.term[slot, pl.ds(pl.multiple_of((2 * k + c) * self.rows, 8), self.rows), column : column + self.width]

    def to_core(self, i, at):
        if i >= 2:
            self.copy(i - 2, 0).wait_send()

        @pl.loop(0, 8)
        def _(k):
            self.c_out[i % 2, k] = self.block(k, 1 - self.c, at).astype(bf16)

        self.copy(i, 0).start()

    def places(self, i, stage, side):
        order = self.order(i)
        left = sorted(order[stage - 1 :])
        bit = order[stage - 1]
        mine = self.bits[bit]
        want = mine if side == 0 else 1 - mine
        rest = [b for b in left if b != bit]
        out = []
        for n in range(2 ** len(rest)):
            value = {b: (n >> (len(rest) - 1 - j)) & 1 for j, b in enumerate(rest)}
            value[bit] = want
            k = 0
            for b in left:
                k = k * 2 + value[b]
            out.append(k)
        return out

    def to_chip(self, i, stage, at=None):
        s, before, came = self.slot(i, stage), self.slot(i, stage - 1), self.landing(i, stage - 1)
        if i >= self.lag[stage - 1]:
            self.copy(i - self.lag[stage - 1], stage).wait_send()
        self.copy(i, stage - 1).wait_recv()

        def value(k):
            if stage == 1:
                return self.block(k, self.c, at) + self.c_in[came, k].astype(f32)
            return self.keep[stage - 2][before, k] + self.into[stage - 2][came, k].astype(f32)

        for n, k in enumerate(self.places(i, stage, 1)):
            self.out[stage - 1][s, n] = value(k).astype(bf16)
        for n, k in enumerate(self.places(i, stage, 0)):
            self.keep[stage - 1][s, n] = value(k)
        self.copy(i, stage).start()

    def total(self, i):
        self.copy(i, 3).wait_recv()
        return self.keep[2][self.slot(i, 3), 0] + self.into[2][self.landing(i, 3), 0].astype(f32)

    def finish(self, count):
        for stage in range(4):
            for i in range(max(count - (2 if stage == 0 else self.lag[stage - 1]), 0), count):
                self.copy(i, stage).wait_send()


class Pipe:
    def __init__(self):
        self.now, self.due = 0, {}

    def at(self, later, stage, item):
        self.due.setdefault(self.now + later, []).append((stage, item))

    def step(self, compute=lambda: None, *item):
        todo = sorted(self.due.pop(self.now, []), key=lambda one: -one[0])
        for stage, (sums, i, place, store) in todo:
            if stage == len(sums.lag) + 1:
                store(sums.total(i).astype(bf16))
            elif stage > 1:
                sums.to_chip(i, stage)
        compute()
        for stage, (sums, i, place, store) in todo:
            if stage == 1:
                sums.to_chip(i, stage, place)
        if item:
            sums, i, place, store = item
            sums.to_core(i, place)
            later = 1
            for stage, lag in enumerate((*sums.lag, None), 1):
                self.at(later, stage, item)
                later += lag or 0
        self.now += 1

    def drain(self):
        while self.due:
            self.step()


BLOCKS, CHUNK, DW, WIDE = 16, 512, 128, 256
WIDE_LAG, DOWN_LAG = (7, 6, 5), (4, 3, 3)


def ffn_phase(pipe, down, wide, dh, given, weights, results, sems, b, bt, m, mt, wg, wu, wd, db, dgate, dup, ends):
    mid_h, b_h, m_h = given[5:]
    _, _, wg_h, wu_h, wd_h = weights
    gd, gg, gu = results[:3]
    in_sem, m_sem, w_sem = sems
    T, D = b.shape
    F = mt.shape[0]
    chunks = [(at, min(CHUNK, F - at)) for at in range(0, F, CHUNK)]
    MT = m.shape[2]

    def w_copies(j):
        s, (at, w) = j % 2, chunks[j]
        pairs = ((wg_h.at[:, pl.ds(at, w)], wg.at[s, :, pl.ds(0, w)]), (wu_h.at[:, pl.ds(at, w)], wu.at[s, :, pl.ds(0, w)]),
                 (wd_h.at[pl.ds(at, w), :], wd.at[s, pl.ds(0, w), :]))
        return [pltpu.make_async_copy(src, dst, w_sem.at[n, s]) for n, (src, dst) in enumerate(pairs)]

    def m_copy(j):
        return pltpu.make_async_copy(m_h.at[:, pl.ds(j * MT, MT)], m.at[j % 2], m_sem.at[j % 2])

    load_b = pltpu.make_async_copy(b_h, b, in_sem.at[0])
    m_copy(0).start()
    m_copy(1).start()
    load_b.start()
    for copy in w_copies(0):
        copy.start()

    def down_term(i):
        def run():
            if i % 2:
                return
            cols = slice(i * DW, (i + 2) * DW)
            if i == 0:
                for j in range(F // MT):
                    m_copy(j).wait()
                    mt[j * MT : (j + 1) * MT, :] = m[j % 2].T
                    if j + 2 < F // MT:
                        m_copy(j + 2).start()

            @tiles(F, F // 5)
            def _(rows):
                down.term[i // 2 % 2, rows, :] = nn(mt[rows, :], dh[:, cols])
        return run

    def down_store(i):
        def run(total):
            gd[:, i * DW : (i + 1) * DW] = total
        return run

    def chunk(j):
        s, (at, w) = j % 2, chunks[j]
        if j == 0:
            load_b.wait()
            bt[...] = b[...].T
        if j + 1 < len(chunks):
            for copy in w_copies(j + 1):
                copy.start()
        for copy in w_copies(j):
            copy.wait()

        @tiles(T)
        def _(rows):
            dm = nt(dh[rows, :], wd[s, :w, :]).astype(bf16).astype(f32)
            gate, up = nn(b[rows, :], wg[s, :, :w]), nn(b[rows, :], wu[s, :, :w])
            sig = 1 / (1 + jnp.exp(-gate))
            to_up = (dm * (gate * sig)).astype(bf16)
            to_gate = (dm * up * (sig * (1 + gate * (1 - sig)))).astype(bf16)
            if w == CHUNK:
                dup[rows, :] = to_up
                dgate[rows, :] = to_gate
            else:
                ends[rows, :w] = to_gate
                ends[rows, w:] = to_up
            term = nt(to_gate, wg[s, :, :w]) + nt(to_up, wu[s, :, :w])
            if j == 0:
                db[rows, :] = term
            else:
                db[rows, :] += term

    def wide_term(j, which, piece, n):
        def run():
            if which == 0 and piece == 0:
                chunk(j)
            right = ends[...] if chunks[j][1] < CHUNK else (dgate, dup)[which][:, piece * WIDE : (piece + 1) * WIDE]

            @tiles(D)
            def _(rows):
                wide.term[n % 2, rows, :] = nn(bt[rows, :], right)
        return run

    def wide_store(j, which, piece):
        at, w = chunks[j]

        def run(total):
            if w < CHUNK:
                gg[:, at : at + w] = total[:, :w]
                gu[:, at : at + w] = total[:, w:]
            else:
                (gg, gu)[which][:, at + piece * WIDE : at + (piece + 1) * WIDE] = total
        return run

    for i in range(D // DW):
        pipe.step(down_term(i), down, i, (i // 2 % 2, i % 2 * DW), down_store(i))
    for j, (at, w) in enumerate(chunks):
        for which, piece in [(which, piece) for which in (0, 1) for piece in range(CHUNK // WIDE)] if w == CHUNK else [(0, 0)]:
            n = wide.count
            wide.count += 1
            pipe.step(wide_term(j, which, piece, n), wide, n, (n % 2, 0), wide_store(j, which, piece))
    mid = b
    load_mid = pltpu.make_async_copy(mid_h, mid, in_sem.at[0])
    load_mid.start()
    load_mid.wait()

    @tiles(T)
    def _(rows):
        g = norm_back(db[rows, :].astype(bf16).astype(f32), mid[rows, :].astype(f32))
        dh[rows, :] = (dh[rows, :].astype(f32) + g.astype(bf16).astype(f32)).astype(bf16)


def stacked(ref, rows, at):
    return jnp.concatenate([ref[rows, at + n * HEAD : at + (n + 1) * HEAD] for n in range(HEADS)], axis=0)


def swapped(t):
    return jnp.concatenate([t[:, HEAD // 2 :], t[:, : HEAD // 2]], axis=1)


def attention_phase(pipe, wide, dmid, given, weights, tables, results, in_sem, a, at, h, qkv, att, att_t, lse, cos, sin, wo, wqkv, delta, dq, dk, dv, da):
    a_h, h_h, qkv_h, att_h, lse_h = given[:5]
    wqkv_h, wo_h = weights[:2]
    go, gqkv = results[3:]
    T, D = a.shape
    datt, dqkv = a, qkv
    pairs = ((att_h, att), (a_h, a), (wo_h, wo), (lse_h, lse), (qkv_h, qkv), (tables[0], cos), (tables[1], sin), (wqkv_h, wqkv), (h_h, h))
    loads = [pltpu.make_async_copy(src, dst, in_sem.at[n]) for n, (src, dst) in enumerate(pairs)]
    for load in loads:
        load.start()
    for load in loads[:3]:
        load.wait()
    att_t[...] = att[...].T
    at[...] = a[...].T

    def term(left, right, n):
        @tiles(D)
        def _(rows):
            wide.term[n % 2, rows, :] = nn(left[rows, :], right)

    def o_item(piece):
        n = wide.count
        wide.count += 1
        cols = slice(piece * WIDE, (piece + 1) * WIDE)

        def store(total):
            go[:, cols] = total
        return (lambda: term(att_t, dmid[:, cols], n)), wide, n, (n % 2, 0), store

    def from_o():
        @tiles(T)
        def _(rows):
            datt[rows, :] = nt(dmid[rows, :], wo[...]).astype(bf16)

        for n in range(HEADS * GROUPS):
            cols = slice(n * HEAD, (n + 1) * HEAD)
            product = datt[:, cols].astype(f32) * att[:, cols].astype(f32)
            delta[n : n + 1, :] = product.T.sum(0, keepdims=True)
        for load in loads[3:]:
            load.wait()

    def queries(g, iq):
        def run():
            rows = slice(iq * BQ, (iq + 1) * BQ)
            first = g * PART
            q, d_out = stacked(qkv, rows, first), stacked(datt, rows, g * HEADS * HEAD)
            row = lambda ref: jnp.concatenate([ref[g * HEADS + n : g * HEADS + n + 1, rows] for n in range(HEADS)], axis=1)
            bottom, less = row(lse) * LOG2E, row(delta)
            if iq == 0:
                dk[...] = jnp.zeros_like(dk)
                dv[...] = jnp.zeros_like(dv)
            dq[...] = jnp.zeros_like(dq)
            strip = 2 * BQ

            def keys(j, masked):
                here = pl.ds(pl.multiple_of(j * BQ, BQ), BQ)
                k, v = qkv[here, first + V_AT - HEAD : first + V_AT], qkv[here, first + V_AT : first + PART]
                for n in range(0, HEADS * BQ, strip):
                    qs, ds = q[n : n + strip], d_out[n : n + strip]
                    p = jnp.exp2(nt(k, qs) * (SCALE * LOG2E) - bottom[:, n : n + strip])
                    if masked:
                        gap = lax.rem(lax.broadcasted_iota(jnp.int32, p.shape, 1), BQ) - lax.broadcasted_iota(jnp.int32, p.shape, 0)
                        p = jnp.where(gap >= 0, p, 0.0)
                    dp = (p * (nt(v, ds) - less[:, n : n + strip])).astype(bf16)
                    dv[here, :] += nn(p.astype(bf16), ds)
                    dk[here, :] += nn(dp, qs)
                    dq[:, n : n + strip] += tn(k, dp)

            if iq:
                pl.loop(0, iq)(lambda j: keys(j, False))
            keys(iq, True)
            back = lambda t, where: t * cos[where, :] + swapped(t) * -sin[where, :]
            low = lambda t: (t * SCALE).astype(bf16).astype(f32)
            for n in range(HEADS):
                dqkv[rows, first + n * HEAD : first + (n + 1) * HEAD] = back(low(dq[:, n * BQ : (n + 1) * BQ].T), rows).astype(bf16)
            if iq == T // BQ - 1:
                every = slice(0, T)
                dqkv[:, first + V_AT - HEAD : first + V_AT] = back(low(dk[...]), every).astype(bf16)
                dqkv[:, first + V_AT : first + PART] = dv[...].astype(bf16)
        return run

    def qkv_item(g, piece):
        n = wide.count
        wide.count += 1
        cols = slice(g * PART + piece * WIDE, g * PART + (piece + 1) * WIDE)

        def run():
            term(at, dqkv[:, cols], n)

        def store(total):
            gqkv[:, cols] = total
        return run, wide, n, (n % 2, 0), store

    def to_a(g):
        def run():
            @tiles(T)
            def _(rows):
                more = nt(dqkv[rows, g * PART : (g + 1) * PART], wqkv[:, g * PART : (g + 1) * PART])
                if g == 0:
                    da[rows, :] = more
                else:
                    g32 = norm_back((da[rows, :] + more).astype(bf16).astype(f32), h[rows, :].astype(f32))
                    dmid[rows, :] = (dmid[rows, :].astype(f32) + g32.astype(bf16).astype(f32)).astype(bf16)
        return run

    for piece in range(D // WIDE):
        pipe.step(*o_item(piece))
    pipe.step(from_o)
    for g in range(GROUPS):
        for iq in range(T // BQ):
            pipe.step(queries(g, iq))
        for piece in range(PART // WIDE):
            pipe.step(*qkv_item(g, piece))
        pipe.step(to_a(g))


def backward_kernel(*refs):
    take = iter(refs)
    some = lambda count: [next(take) for _ in range(count)]
    dy_h, *tables = some(3)
    given, weights = some(8), some(5)
    dx_h, *outs = some(6)
    dh = next(take)
    results = some(5)
    *sems, out_sem = some(4)
    T, D = dh.shape
    F = given[-1].shape[1]
    down, wide = Sums(some(Sums.REFS), F // BLOCKS, DW, DOWN_LAG), Sums(some(Sums.REFS), D // BLOCKS, WIDE, WIDE_LAG)
    load = pltpu.make_async_copy(dy_h, dh, out_sem.at[0])
    load.start()
    down.greet()
    load.wait()
    pipe = Pipe()
    v = lambda *s: pltpu.VMEM(s, bf16)
    w = lambda *s: pltpu.VMEM(s, f32)
    two = lambda *s: v(2, *s)
    pl.run_scoped(
        functools.partial(ffn_phase, pipe, down, wide, dh, given, weights, results, sems),
        v(T, D), v(D, T), two(T, HEAD), v(F, T), two(D, CHUNK), two(D, CHUNK), two(CHUNK, D), w(T, D), v(T, CHUNK), v(T, CHUNK), v(T, WIDE),
    )
    pl.run_scoped(
        functools.partial(attention_phase, pipe, wide, dh, given, weights, tables, results, sems[0]),
        v(T, D), v(D, T), v(T, D), v(*given[2].shape), v(T, D), v(D, T), w(HEADS * GROUPS, T), w(T, HEAD), w(T, HEAD), v(D, D),
        v(*weights[0].shape), w(HEADS * GROUPS, T), w(HEAD, HEADS * BQ), w(T, HEAD), w(T, HEAD), w(T, D),
    )
    out = pltpu.make_async_copy(dh, dx_h, out_sem.at[0])
    out.start()
    pipe.drain()
    copies = [pltpu.make_async_copy(src, dst, out_sem.at[n]) for n, (src, dst) in enumerate(zip(results, outs, strict=True), 1)]
    for copy in copies:
        copy.start()
    down.finish(D // DW)
    wide.finish(wide.count)
    for copy in [out, *copies]:
        copy.wait()


def backward(dy, cos, sin, saved, full, number):
    T, D = dy.shape
    F, P = saved[-1].shape[1], saved[2].shape[1]
    rows, long = D // BLOCKS, F // BLOCKS
    any_ = pl.BlockSpec(memory_space=pl.ANY)
    shapes = [(T, D), (long, D), (rows, F), (rows, F), (rows, D), (rows, P)]
    given = [dy, cos, sin, *saved, *full]
    return pl.pallas_call(
        backward_kernel,
        out_shape=[jax.ShapeDtypeStruct(s, bf16) for s in shapes],
        in_specs=[any_] * len(given),
        out_specs=[any_] * len(shapes),
        scratch_shapes=[*(pltpu.VMEM(s, bf16) for s in shapes), SEM((9,)), SEM((2,)), SEM((3, 2)), SEM((len(shapes),)),
                        *Sums.scratch(long, DW, DOWN_LAG, 2 * DW), *Sums.scratch(rows, WIDE, WIDE_LAG)],
        compiler_params=params(number),
        name="backward",
    )(*given)


LAYERS = 2
AHEAD = 2
ALONG = (1, 2, 0)
MATRICES = ("qkv", "o", "gate", "up", "down")
OVER_X = ("qkv", "gate", "up")


class Gather:
    def __init__(self, srcs, outs, own, sems, halves):
        self.srcs, self.outs, self.own, self.halves = srcs, outs, own, halves
        self.load_sem, self.store_sem, self.send_sem, self.c_sem, self.chip_sem, self.x_sem = sems
        self.x, self.y, self.z, self.c = where_am_i()
        self.bits = chip_bits(self.y, self.z)
        n = len(srcs)
        self.items = [(i, l) for l in range(LAYERS) for i in range(n)]
        self.loads = [pltpu.make_async_copy(srcs[i], own[i], self.load_sem.at[i]) for i in range(n)]

    def begin(self):
        for load in self.loads:
            load.start()
        greet([{"c": 1 - self.c}, {"x": 1 - self.x}] + [partner(self.bits, bit) for bit in range(len(self.bits))])
        for load in self.loads:
            load.wait()

    def part(self, ref, item, part):
        half = self.halves[item[0]]
        return ref if half is None or part is None else ref.at[pl.ds(pl.multiple_of(part * half, half), half)]

    def mine(self, item, part):
        i, l = item
        return self.part(self.own[i].at[l], item, part)

    def block(self, item, flips, part):
        i, l = item
        number = 0
        for bit, value in enumerate(self.bits):
            number = number * 2 + ((1 - value) if bit in flips else value)
        return self.part(self.outs[l][i].at[number * 2 + self.c], item, part)

    def remote(self, item, src, dst, sem, **there):
        i, l = item
        return pltpu.make_async_remote_copy(src, dst, self.send_sem.at[l, i], sem, device_id=peer(**there), device_id_type=pl.DeviceIdType.MESH)

    def pass_on(self, item, src, dst, flips, stage):
        i, l = item
        for bit in ALONG[stage:]:
            self.remote(item, src, dst, self.chip_sem.at[l, i, self.index(item, (*flips, bit))], **partner(self.bits, bit)).start()
        if flips:
            if self.halves[i] is not None:
                self.remote(item, src, dst, self.x_sem.at[l, i, self.index(item, flips)], x=1 - self.x).start()
            self.remote(item, src, dst, self.c_sem.at[l, i], c=1 - self.c).start()

    def index(self, item, flips):
        return sum(2**bit for bit in flips) - 1

    def start(self, item):
        i, l = item
        whole = self.block(item, (), None)
        pltpu.make_async_copy(self.own[i].at[l], whole, self.store_sem.at[l, i]).start()
        self.pass_on(item, self.mine(item, self.x), self.block(item, (), self.x), (), 0)
        self.remote(item, self.own[i].at[l], whole, self.c_sem.at[l, i], c=1 - self.c).start()

    def routes(self, item, stage):
        before, bit = ALONG[:stage], ALONG[stage]
        return [(*(b for n, b in enumerate(before) if mask >> n & 1), bit) for mask in range(2**stage)]

    def from_chips(self, item, stage):
        i, l = item
        for flips in self.routes(item, stage):
            ref = self.block(item, flips, self.x)
            self.remote(item, ref, ref, self.chip_sem.at[l, i, self.index(item, flips)], c=1 - self.c).wait_recv()
            self.pass_on(item, ref, ref, flips, stage + 1)

    def from_group(self, item):
        i, l = item
        if self.halves[i] is not None:
            for stage in range(len(self.bits)):
                for flips in self.routes(item, stage):
                    ref = self.block(item, flips, 1 - self.x)
                    self.remote(item, ref, ref, self.x_sem.at[l, i, self.index(item, flips)], c=1 - self.c).wait_recv()
                    self.remote(item, ref, ref, self.c_sem.at[l, i], c=1 - self.c).start()

    def whole(self, item):
        i, l = item
        half = self.outs[l][i].at[pl.ds(0, 8)]
        self.remote(item, half, half, self.c_sem.at[l, i], c=1 - self.c).wait_recv()
        pltpu.make_async_copy(self.own[i].at[l], self.block(item, (), None), self.store_sem.at[l, i]).wait()

    def finish(self):
        for item in self.items:
            i, l = item
            sent = self.outs[l][i].at[pl.ds(0, 15)]
            self.remote(item, sent, sent, self.c_sem.at[l, i], c=1 - self.c).wait_send()

    def steps(self):
        m, bits = len(self.items), len(self.bits)
        out = [(lambda item=item: self.start(item), None) for item in self.items[:AHEAD]]
        for k in range(m + LAGS[bits]):
            for stage, lag in enumerate(LAGS[:bits]):
                if 0 <= k - lag < m:
                    out.append((lambda item=self.items[k - lag], stage=stage: self.from_chips(item, stage), None))
                if stage == 0 and k + AHEAD < m:
                    out.append((lambda item=self.items[k + AHEAD]: self.start(item), None))
            if 0 <= k - LAGS[bits] < m:
                out.append((lambda item=self.items[k - LAGS[bits]]: self.from_group(item), self.items[k - LAGS[bits]]))
        return out


def forward_kernel(*refs, halves):
    n = len(MATRICES)
    take = iter(refs)
    some = lambda count: [next(take) for _ in range(count)]
    srcs, (x_h, cos_h, sin_h) = some(n), some(3)
    outs = [some(n) for _ in range(LAYERS)]
    kept = [some(8) for _ in range(LAYERS)]
    own, sems = some(n), some(6)
    h, cos, sin, wqkv, wo, a, qkv, att, lse, mid, b, m, acc, wg, wu, wd, in_sem, w_sem, out_sem = take
    T, D = h.shape
    F = m.shape[1]
    chunks = [(at, min(CHUNK, F - at)) for at in range(0, F, CHUNK)]
    net = Gather(srcs, outs, own, sems, halves)
    tables = [pltpu.make_async_copy(src, dst, in_sem.at[k]) for k, (src, dst) in enumerate(((x_h, h), (cos_h, cos), (sin_h, sin)))]
    for copy in tables:
        copy.start()
    net.begin()
    pieces = []
    add = lambda l, *need: lambda run: pieces.append(([(MATRICES.index(name), l) for name in need], run))
    flat = lambda l, name: outs[l][MATRICES.index(name)]
    saved = lambda l, k, src: pltpu.make_async_copy(src, kept[l][k], out_sem.at[k])
    flow = dict(enumerate((a, h, qkv, att, lse, mid, b, m)))

    def rows_of(w_h, at, w):
        return w_h.at[:, :, pl.ds(at, w)]

    def w_copies(l, j):
        s, (at, w) = j % 2, chunks[j]
        pairs = ((rows_of(flat(l, "gate"), at, w), wg.at[s, :, :, pl.ds(0, w)]), (rows_of(flat(l, "up"), at, w), wu.at[s, :, :, pl.ds(0, w)]))
        return [pltpu.make_async_copy(src, dst, w_sem.at[k, s]) for k, (src, dst) in enumerate(pairs)]

    def d_copy(l, j):
        return pltpu.make_async_copy(flat(l, "down").at[pl.ds(2 * j, 2)], wd.at[j % 2], w_sem.at[2, j % 2])

    for l in range(LAYERS):
        qkv_in = pltpu.make_async_copy(flat(l, "qkv"), wqkv, in_sem.at[3])
        o_in = pltpu.make_async_copy(flat(l, "o"), wo, in_sem.at[4])

        @add(l, "qkv")
        def _(l=l, qkv_in=qkv_in):
            qkv_in.start()
            if l == 0:
                for copy in tables:
                    copy.wait()
            else:
                saved(0, 0, a).wait()
                saved(0, 2, qkv).wait()
                saved(l, 1, h).start()

        @add(l, "qkv")
        def _(l=l, qkv_in=qkv_in):
            qkv_in.wait()
            w = wqkv[...].reshape(D, GROUPS * PART)

            @tiles(T)
            def _(rows):
                a[rows, :] = norm(h[rows, :].astype(f32))
                for g in range(GROUPS):
                    first = g * PART
                    got = nn(a[rows, :], w[:, first : first + PART]).astype(bf16)
                    for k in range(HEADS + 1):
                        t = got[:, k * HEAD : (k + 1) * HEAD].astype(f32)
                        qkv[rows, first + k * HEAD : first + (k + 1) * HEAD] = (t * cos[rows, :] + swapped(t) * sin[rows, :]).astype(bf16)
                    qkv[rows, first + V_AT : first + PART] = got[:, V_AT:]

            saved(l, 0, a).start()
            saved(l, 2, qkv).start()
            if l:
                saved(0, 3, att).wait()
                saved(0, 4, lse).wait()

        for iq in range(T // BQ):
            @add(l, "qkv")
            def _(iq=iq):
                attend_block(qkv, att, lse, iq)

        @add(l, "o")
        def _(l=l, o_in=o_in):
            o_in.start()
            saved(l, 3, att).start()
            saved(l, 4, lse).start()
            if l:
                saved(0, 5, mid).wait()
                saved(0, 6, b).wait()

        @add(l, "o")
        def _(l=l, o_in=o_in):
            o_in.wait()
            w = wo[...].reshape(D, D)

            @tiles(T)
            def _(rows):
                mid[rows, :] = (h[rows, :].astype(f32) + nn(att[rows, :], w).astype(bf16).astype(f32)).astype(bf16)
                b[rows, :] = norm(mid[rows, :].astype(f32))

            saved(l, 5, mid).start()
            saved(l, 6, b).start()

        @add(l, "gate", "up")
        def _(l=l):
            for copy in w_copies(l, 0):
                copy.start()
            if l:
                saved(0, 7, m).wait()

        for j, (at, w) in enumerate(chunks):
            @add(l, "gate", "up")
            def _(l=l, j=j, at=at, w=w):
                if j + 1 < len(chunks):
                    for copy in w_copies(l, j + 1):
                        copy.start()
                for copy in w_copies(l, j):
                    copy.wait()
                left, right = (t[j % 2, :, :, :w].reshape(D, w) for t in (wg, wu))

                @tiles(T)
                def _(rows):
                    gate, up = nn(b[rows, :], left), nn(b[rows, :], right)
                    m[rows, at : at + w] = (gate * (1 / (1 + jnp.exp(-gate))) * up).astype(bf16)

        @add(l, "gate", "up")
        def _(l=l):
            saved(l, 7, m).start()

        if l + 1 < LAYERS:
            @add(l, "down")
            def _(l=l):
                d_copy(l, 0).start()

            wide = F // 8
            for j in range(8):
                @add(l, "down")
                def _(l=l, j=j):
                    if j < 7:
                        d_copy(l, j + 1).start()
                    d_copy(l, j).wait()
                    w = wd[j % 2].reshape(wide, D)

                    @tiles(T)
                    def _(rows):
                        acc[rows, :] = nn(m[rows, j * wide : (j + 1) * wide], w) + (acc[rows, :] if j else 0.0)

            @add(l, "down")
            def _():
                @tiles(T)
                def _(rows):
                    h[rows, :] = (mid[rows, :].astype(f32) + acc[rows, :].astype(bf16).astype(f32)).astype(bf16)

    arrived, waited = set(), set()

    def ready(need):
        return all(item in arrived for item in need)

    def do_piece():
        need, run = pieces.pop(0)
        for item in need:
            if item not in waited:
                net.whole(item)
                waited.add(item)
        run()

    for run, item in net.steps():
        run()
        if item is not None:
            arrived.add(item)
        for _ in range(PER_STEP):
            if pieces and ready(pieces[0][0]):
                do_piece()
    while pieces:
        do_piece()
    for item in net.items:
        if item not in waited:
            net.whole(item)
    net.finish()
    for k, src in flow.items():
        saved(LAYERS - 1, k, src).wait()


def forward(blocks, x, cos, sin):
    n = len(blocks)
    T, D = x.shape
    rows = D // BLOCKS
    F, P = blocks[2].shape[2], blocks[0].shape[2]
    halves = [b.shape[1] // 2 if name in OVER_X else None for name, b in zip(MATRICES, blocks, strict=True)]
    any_ = pl.BlockSpec(memory_space=pl.ANY)
    v = lambda *s: pltpu.VMEM(s, bf16)
    w = lambda *s: pltpu.VMEM(s, f32)
    shape = lambda *s: jax.ShapeDtypeStruct(s, bf16)
    stats = jax.ShapeDtypeStruct((HEADS * GROUPS, T), f32)
    kept = [shape(T, D), shape(T, D), shape(T, P), shape(T, D), stats, shape(T, D), shape(T, D), shape(T, F)]
    outs = [shape(BLOCKS, *b.shape[1:]) for b in blocks] * LAYERS + kept * LAYERS
    got = pl.pallas_call(
        functools.partial(forward_kernel, halves=halves),
        out_shape=outs,
        in_specs=[any_] * (n + 3),
        out_specs=[any_] * len(outs),
        scratch_shapes=[
            *(pltpu.VMEM(b.shape, bf16) for b in blocks),
            SEM((n,)), *(SEM((LAYERS, n)),) * 3, *(SEM((LAYERS, n, 7)),) * 2,
            v(T, D), w(T, HEAD), w(T, HEAD), v(BLOCKS, rows, P), v(BLOCKS, rows, D), v(T, D), v(T, P), v(T, D), w(*stats.shape), v(T, D), v(T, D), v(T, F), w(T, D),
            *(v(2, BLOCKS, rows, CHUNK),) * 2, v(2, 2, F // BLOCKS, D), SEM((5,)), SEM((3, 2)), SEM((8,)),
        ],
        compiler_params=params(1),
        name="gather_and_forward",
    )(*blocks, x, cos, sin)
    full = [[w.reshape(-1, w.shape[2]) for w in got[l * n : (l + 1) * n]] for l in range(LAYERS)]
    rest = got[LAYERS * n :]
    return full, [list(rest[l * 8 : (l + 1) * 8]) for l in range(LAYERS)]


THETA = 10000


def turns(tokens):
    half = HEAD // 2
    power = THETA ** (-np.arange(half, dtype=np.float32) / np.float32(half))
    angle = np.arange(tokens, dtype=np.float32)[:, None] * power.astype(np.float32)
    cos, sin = np.cos(angle), np.sin(angle)
    return jnp.asarray(np.concatenate([cos, cos], 1), f32), jnp.asarray(np.concatenate([-sin, sin], 1), f32)


def by_key_head(wq, wk, wv):
    q = HEADS * HEAD
    return jnp.concatenate([w[:, :, g * n : (g + 1) * n] for g in range(GROUPS) for w, n in ((wq, q), (wk, HEAD), (wv, HEAD))], axis=2)


def by_kind(t):
    q = HEADS * HEAD
    spans = ((0, q), (q, q + HEAD), (q + HEAD, PART))
    return [jnp.concatenate([t[:, g * PART + a : g * PART + b] for g in range(GROUPS)], axis=1) for a, b in spans]


def solution(mesh):
    fine = jax.sharding.Mesh(mesh.devices.reshape(2, 2, 4, 2), ("x", "y", "z", "c"))

    def step(x, dy, wq, wk, wv, wo, w_gate, w_up, w_down):
        cos, sin = turns(x.shape[1])
        full, saved = forward([by_key_head(wq, wk, wv), wo, w_gate, w_up, w_down], x[0], cos, sin)
        saved[0][1] = x[0]
        dh, grads = dy[0], []
        for number in reversed(range(LAYERS)):
            dh, down, gate, up, by_o, by_qkv = backward(dh, cos, sin, saved[number], full[number], 2 + number)
            grads.insert(0, (*by_kind(by_qkv), by_o, gate, up, down))
        return (dh[None], *(jnp.stack(same) for same in zip(*grads, strict=True)))

    group = ("y", "z", "c")
    states, cut = P(("x", *group), None, None), P(None, group, None)
    return jax.shard_map(
        step,
        mesh=fine,
        in_specs=(states, states) + (cut,) * 7,
        out_specs=(states,) + (P("x", group, None),) * 7,
        check_vma=False,
    )
```
